128 devices in a mesh: rows: 32 (over y, z, core), chan: 4 (over x).
Axes of the slice: x: 4, y: 4, z: 4, core: 2. Of those that a mesh axis runs over, the one named last changes fastest.
Arguments:
- radiances: float32 [16, 65536], P('chan', 'rows'), may hold values from -6 to 6
- band: int32 [65536, 1], P('rows'), may hold values from 0 to 31; in each aligned block of 2048 rows (0 to 2047, 2048 to 4095, ...) at most 128 rows name the same one
- row_in_band: int32 [65536], P('rows'), may hold values from 0 to 3
- column: int32 [65536], P('rows'), may hold values from 0 to 1439
Outputs:
- cell_count: int32 [128, 1440], P('rows')
- cell_mean: float32 [16, 128, 1440], P('chan', 'rows')
- cell_var: float32 [16, 128, 1440], P('chan', 'rows')
- cell_spread: float32 [128, 1440], P('rows')
- departure: float32 [16, 65536], P('chan', 'rows')
The draws below stay inside these ranges and needn't reach their ends.
Inputs may be any that keep to these rules, and one draw needn't show every extreme that they name: Within each aligned block of 2048 observations (one scan-time shard) no band is named by more than 128 observations, and in some blocks one band is named by exactly 128.
All inputs are finite; a program needn't handle non-finite values.
Results may differ from the reference program's by a relative error of at most 0.0003.
Values sent between devices are 32-bit elements.
A program may use at most 64 MiB of HBM per device.

```python
import math
import jax
import jax.numpy as jnp
import numpy as np
from jax import lax

CHAN = 16
COLS = 1440
ROWS_DEV = 4
OBS_DEV = 2048
LATS = 128
OBS = 65536
CAP = 128
N_ROWS = 32


def touch_ends(result, key, smallest, high):
    index_at = [jax.random.randint(jax.random.fold_in(key, axis), (), 0, length) for axis, length in enumerate(result.shape)]
    longest = result.shape.index(max(result.shape))
    neighbour = index_at[:longest] + [(index_at[longest] + 1) % result.shape[longest]] + index_at[longest + 1:]
    return result.at[tuple(index_at)].set(smallest).at[tuple(neighbour)].set(high)


def shard_levels(rng, shape, cuts, smallest, top_value):
    def one(dim, parts):
        draws = jax.random.uniform(jax.random.fold_in(jax.random.fold_in(rng, 6), dim), (parts,), jnp.float32, smallest / len(cuts), top_value / len(cuts))
        return jnp.repeat(jnp.exp(draws), shape[dim] // parts).reshape((-1,) + (1,) * (len(shape) - dim - 1))

    level = one(*cuts[0])
    for cut in cuts[1:]:
        level = level * one(*cut)
    return level


def shared_out(key, own, number, rows, number_of, top, reach, lean):
    sequence = jax.random.permutation(key, number_of)
    crowded, ordinary = portions_of(number_of, rows * top, reach, lean, True), portions_of(number_of, rows * top, reach, lean, False)
    places = jnp.arange(number_of)

    def named(sizes, turn):
        used = int((sizes > 0).sum())
        fixed = max(1, used // 4)
        passed = fixed + (places - fixed + turn * (used - fixed)) % max(1, number_of - fixed)
        return jnp.zeros((number_of,), jnp.int32).at[sequence[jnp.where(places < fixed, places, passed)]].set(jnp.asarray(sizes, jnp.int32))

    sizes = jnp.where(number % 4 == 0, named(crowded, number // 4), named(ordinary, number - number // 4 - 1))
    mixed = jax.random.permutation(jax.random.fold_in(own, 3), number_of)
    source_of, sink = mixed[0:number_of // 2 * 2:2], mixed[1:number_of // 2 * 2:2]
    margin = jnp.minimum(sizes[source_of] - 1, reach - sizes[sink]) // 2
    margin = jnp.where((source_of == sequence[0]) | (sink == sequence[0]) | (sizes[sink] == 0), 0, jnp.maximum(margin, 0))
    passed = jax.random.randint(jax.random.fold_in(own, 4), (number_of // 2,), 0, 1 << 20) % (margin + 1)
    sizes = sizes.at[source_of].add(-passed).at[sink].add(passed)
    labels = jnp.searchsorted(jnp.cumsum(sizes), jnp.arange(rows * top), side="right").astype(jnp.int32)
    grid = labels.reshape(top, rows).T
    grid = grid[jax.random.permutation(jax.random.fold_in(own, 1), rows)]
    turn = jax.random.randint(jax.random.fold_in(own, 2), (rows, 1), 0, top)
    return jnp.take_along_axis(grid, (jnp.arange(top)[None, :] + turn) % top, axis=1)


def portions_of(count, total, limit, lean, full):
    weights = [(1 << 20) // math.isqrt(rank ** lean) + 1 for rank in range(1, count + 1)]
    largest = limit if full else min(limit, max(-(-total // count), total * weights[0] // sum(weights)))
    least = 1 if total - largest >= count - 1 else 0
    counts, surplus = [largest] + [least] * (count - 1), total - largest - least * (count - 1)
    while surplus > 0:
        free = [i for i in range(1, count) if counts[i] < largest] or [i for i in range(1, count) if counts[i] < limit]
        pool, budget = sum([weights[i] for i in free]), surplus
        for i in free:
            addition = min(limit - counts[i], max(1, budget * weights[i] // pool), surplus)
            counts[i] = counts[i] + addition
            surplus = surplus - addition
    return np.array(counts)


def noise(own_key, extent, deviation, most, shards=(), held_as=jnp.bfloat16):
    level = shard_levels(own_key, extent, shards, -0.22, 0.18) if shards else 1.0
    values = jax.random.normal(own_key, extent, jnp.float32) * deviation * level
    return jnp.minimum(jnp.maximum(values, -most), most).astype(held_as)


def setup_inputs(seed: int = 0) -> dict:
    arg_keys = jax.random.split(jax.random.key(seed), 5)
    radiances = noise(arg_keys[0], (CHAN, OBS), 1.0, 6.0, ((0, 4), (1, 32)), jnp.float32)
    band_keys = jax.random.split(jax.random.fold_in(arg_keys[1], 1), OBS // OBS_DEV)
    band_turns = jax.random.permutation(jax.random.fold_in(arg_keys[1], 3), OBS // OBS_DEV)
    band = jax.vmap(lambda own, number: shared_out(jax.random.fold_in(arg_keys[1], 2), own, number, OBS_DEV, N_ROWS, 1, CAP, 2))(band_keys, band_turns).reshape((OBS, 1))
    row_in_band = touch_ends(jax.random.randint(arg_keys[2], (OBS,), 0, ROWS_DEV), jax.random.fold_in(arg_keys[2], 1), 0, ROWS_DEV - 1).astype(jnp.int32)
    column = touch_ends(jax.random.randint(arg_keys[3], (OBS,), 0, COLS), jax.random.fold_in(arg_keys[3], 1), 0, COLS - 1).astype(jnp.int32)
    return {"radiances": radiances, "band": band, "row_in_band": row_in_band, "column": column}


def reference(radiances, band, row_in_band, column):
    lat = band[:, 0] * ROWS_DEV + row_in_band
    cell = (lat * COLS + column).astype(jnp.int32)
    cells = LATS * COLS
    ones = jnp.ones(cell.shape, jnp.float32)
    count = jax.ops.segment_sum(ones, cell, num_segments=cells)
    values = radiances.astype(jnp.float32).T
    first = jax.ops.segment_sum(values, cell, num_segments=cells)
    second = jax.ops.segment_sum(values * values, cell, num_segments=cells)
    denom = jnp.maximum(count, 1.0)[:, None]
    mean = first / denom
    var = jnp.maximum(second / denom - mean * mean, 0.0)
    spread = lax.optimization_barrier(jnp.sum(var, axis=1))
    scale = lax.rsqrt(1.0 + spread / CHAN)
    departure = (radiances - mean[cell].T) * scale[cell][None, :]
    cell_count = count.reshape(LATS, COLS).astype(jnp.int32)
    cell_mean = mean.T.reshape(CHAN, LATS, COLS)
    cell_var = var.T.reshape(CHAN, LATS, COLS)
    return (cell_count, cell_mean, cell_var, spread.reshape(LATS, COLS), departure)
```

```python
import functools

import jax
import jax.numpy as jnp
from jax import lax
from jax.experimental import pallas as pl
from jax.experimental.pallas import tpu as pltpu
from jax.sharding import PartitionSpec as P

CHAN = 16
COLS = 1440
NROW = 32
NCHAN = 4
CH = 4
OBS = 2048
CAP = 128
WIDE = 256
NCELL = 24
MESH = pl.DeviceIdType.MESH
F32 = jnp.float32
BF16 = jnp.bfloat16


def hops(offset):
    ring = (0, 1, 2, 1)
    return ring[offset >> 3] + ring[(offset >> 1) & 3]


NEAR = tuple(sorted(range(NROW), key=hops))
FAR = tuple(d for d in reversed(NEAR) if d)
GROUPS = (NEAR[:16], NEAR[16:])


def iota(shape, dim):
    return lax.broadcasted_iota(jnp.int32, shape, dim)


def rows16(row):
    return jnp.broadcast_to(row, (16, row.shape[1])).astype(BF16)


def count16(lanes):
    return iota((16, lanes), 0).astype(F32).astype(BF16)


def hot_into(ref, top, cols, names, blocks, lanes, first=0):
    one, zero = jnp.ones((16, lanes), BF16), jnp.zeros((16, lanes), BF16)
    steps = count16(lanes)
    for k in range(blocks):
        ref[top + 16 * k : top + 16 * k + 16, cols] = jnp.where(
            names == steps + jnp.asarray(16 * k + first, BF16), one, zero
        )


def high_of(x):
    return x.astype(BF16).astype(F32)


def spread_into_slots(radiances, bands, rib, column, left, right, rank_ref, tiles):
    lanes = OBS
    names = rows16(bands)
    hot_into(right, 0, slice(0, lanes), names, 2, lanes)
    blocks = [right[0:32, WIDE * j : WIDE * j + WIDE] for j in range(OBS // WIDE)]
    before, seen = [], jnp.zeros((32, WIDE), BF16)
    for block in blocks:
        before.append(seen)
        seen = seen + block
    stacked = jnp.concatenate(
        [jnp.concatenate(before, axis=0), jnp.concatenate(blocks, axis=0)], axis=1
    )
    ones = jnp.ones((WIDE, WIDE), BF16)
    upper = jnp.where(iota((WIDE, WIDE), 0) <= iota((WIDE, WIDE), 1), 1.0, 0.0).astype(BF16)
    prefix = jnp.dot(
        stacked, jnp.concatenate([ones, upper], axis=0), preferred_element_type=F32
    )
    ranks = []
    for j, block in enumerate(blocks):
        own = block.astype(F32) * prefix[32 * j : 32 * j + 32]
        ranks.append(jnp.sum(own, axis=0, keepdims=True) - 1.0)
    rank = jnp.concatenate(ranks, axis=1)
    rank_ref[...] = rank
    hot_into(right, 0, slice(0, lanes), rows16(rank), CAP // 16, lanes)

    row = iota((8, lanes), 0)
    both = jnp.concatenate([radiances, radiances], axis=0)
    high = high_of(both)
    middle = high_of(both - high)
    low = both - high - middle
    cell_hi = jnp.broadcast_to(((column >> 8) * 4 + rib + 1).astype(F32), (8, lanes))
    cell_lo = jnp.broadcast_to((column & 255).astype(F32), (8, lanes))
    names_of = jnp.where(row == 4, cell_hi, jnp.where(row == 5, cell_lo, 0.0))
    payload = jnp.concatenate(
        [jnp.where(row < 4, high, middle), jnp.where(row < 4, low, names_of)], axis=0
    ).astype(BF16)
    zero = jnp.zeros((16, lanes), BF16)
    for b in range(NROW):
        left[16 * b : 16 * b + 16, :] = jnp.where(names == jnp.asarray(b, BF16), payload, zero)
    placed = lax.dot_general(
        left[...], right[...], (((1,), (1,)), ((), ())), preferred_element_type=F32
    ).reshape(NROW, 16, CAP)
    upper_half, lower_half = placed[:, :8], placed[:, 8:]
    tile_row = iota((NROW, 8, CAP), 1)
    total = upper_half + pltpu.roll(upper_half, 4, 1) + lower_half
    tiles[...] = jnp.where(tile_row < 4, total, lower_half)


def comm_kernel(
    rad_ref,
    band_ref,
    rib_ref,
    col_ref,
    ret_ref,
    rank_ref,
    brel_ref,
    mean_ref,
    var_ref,
    count_ref,
    spread_ref,
    left,
    right,
    tiles,
    arrived,
    features,
    hot,
    sums,
    table,
    back,
    returned,
    partial,
    spreads,
    send_sem,
    recv_sem,
    ready_sem,
):
    me, mine = lax.axis_index("rows"), lax.axis_index("chan")
    peer = {d: lax.bitwise_xor(me, d) for d in range(NROW)}
    other = {k: lax.bitwise_xor(mine, k) for k in range(NCHAN)}
    barrier = pltpu.get_barrier_semaphore()
    for d in FAR:
        pl.semaphore_signal(barrier, 1, device_id={"rows": peer[d]}, device_id_type=MESH)
    for k in range(1, NCHAN):
        pl.semaphore_signal(barrier, 1, device_id={"chan": other[k]}, device_id_type=MESH)

    bands = lax.bitwise_xor(band_ref[...], me).astype(F32)
    brel_ref[...] = bands
    spread_into_slots(
        rad_ref[...], bands, rib_ref[...], col_ref[...], left, right, rank_ref, tiles
    )
    arrived[0] = tiles[0]
    pl.semaphore_wait(barrier, NROW - 1 + NCHAN - 1)

    def remote(src, dst, which, **to):
        return pltpu.make_async_remote_copy(
            src_ref=src,
            dst_ref=dst,
            send_sem=send_sem.at[which],
            recv_sem=recv_sem.at[which],
            device_id=to,
            device_id_type=MESH,
        )

    for d in FAR:
        which = 0 if d in GROUPS[0] else 1
        remote(
            tiles.at[d, pl.ds(0, 6)], arrived.at[d, pl.ds(0, 6)], which, rows=peer[d]
        ).start()
    for k in range(1, NCHAN):
        pl.semaphore_signal(ready_sem, 1, device_id={"chan": other[k]}, device_id_type=MESH)

    for g, group in enumerate(GROUPS):
        n = len(group)
        lanes = n * CAP
        cols = slice(g * lanes, (g + 1) * lanes)
        waited = arrived.at[pl.ds(0, n - (0 in group)), pl.ds(0, 6)]
        remote(waited, waited, g, rows=me).wait()
        row = iota((8, lanes), 0)
        tile = jnp.concatenate([arrived[d] for d in group], axis=1)
        value = jnp.where(row < 4, tile, pltpu.roll(tile, 4, 0))
        square = value * value
        value_hi, square_hi = high_of(value), high_of(square)
        feature = jnp.concatenate(
            [
                jnp.where(row < 4, value_hi, value - value_hi),
                jnp.where(row < 4, square_hi, square - square_hi),
            ],
            axis=0,
        ).astype(BF16)
        cell_hi = rows16(jnp.concatenate([arrived[d, 4:5] for d in group], axis=1))
        cell_lo = rows16(jnp.concatenate([arrived[d, 5:6] for d in group], axis=1))
        zero = jnp.zeros((16, lanes), BF16)
        for a in range(NCELL):
            features[16 * a : 16 * a + 16, :] = jnp.where(
                cell_hi == jnp.asarray(a + 1, BF16), feature, zero
            )
        hot_into(features, 16 * NCELL, slice(0, lanes), cell_hi, 2, lanes, first=1)
        hot_into(hot, 0, cols, cell_lo, WIDE // 16, lanes)
        part = lax.dot_general(
            features[...], hot[:, cols], (((1,), (1,)), ((), ())), preferred_element_type=F32
        )
        for half in range(2):
            piece = part[:, CAP * half : CAP * half + CAP]
            if g == 0:
                sums[half] = piece
            else:
                sums[half] += piece

    def both_halves(pick):
        return jnp.concatenate([sums[half, pick, :] for half in range(2)], axis=1)

    count = both_halves(slice(16 * NCELL, 16 * NCELL + NCELL))
    inverse = 1.0 / jnp.maximum(count, 1.0)
    means, variances = [], []
    for c in range(CH):
        pick = lambda f: both_halves(pl.ds(f, NCELL, stride=16))
        mean = (pick(c) + pick(c + 4)) * inverse
        var = jnp.maximum((pick(c + 8) + pick(c + 12)) * inverse - mean * mean, 0.0)
        means.append(mean)
        variances.append(var)
    own_spread = (variances[0] + variances[1]) + (variances[2] + variances[3])
    spreads[0] = own_spread
    fields = means + [own_spread]
    highs = [high_of(x) for x in fields]
    lows = [x - h for x, h in zip(fields, highs)]
    table[...] = jnp.concatenate(highs + lows, axis=0).astype(BF16)

    nfield = len(fields)
    order = [d for group in GROUPS for d in group]
    turn = 4
    for t in reversed(range(NROW // turn)):
        group = order[turn * t : turn * t + turn]
        lanes = turn * CAP
        found = jnp.dot(
            table[...], hot[:, lanes * t : lanes * t + lanes], preferred_element_type=F32
        ).reshape(2 * nfield, NCELL, lanes)
        found = found[:nfield] + found[nfield:]
        cell_hi = jnp.concatenate([arrived[d, 4:5] for d in group], axis=1)
        here = jnp.broadcast_to(cell_hi, (NCELL, lanes)) == (iota((NCELL, lanes), 0) + 1).astype(F32)
        row = iota((8, lanes), 0)
        looked = jnp.zeros((8, lanes), F32)
        for f in range(nfield):
            only = jnp.where(here, found[f], 0.0)
            only = only[0:8] + only[8:16] + only[16:24]
            only = only + pltpu.roll(only, 4, 0)
            only = only + pltpu.roll(only, 2, 0)
            only = only + pltpu.roll(only, 1, 0)
            looked = jnp.where(row == f, only, looked)
        tile = jnp.concatenate([arrived[d] for d in group], axis=1)
        tile = jnp.where(row < 4, tile - looked, looked)
        for i, d in enumerate(group):
            back[d] = tile[:, CAP * i : CAP * i + CAP]
        if t == NROW // turn - 1:
            pl.semaphore_wait(ready_sem, NCHAN - 1)
        for d in reversed(group):
            for k in (2, 1, 3):
                remote(
                    back.at[d, pl.ds(4, 1)],
                    partial.at[k, pl.ds(d, 1)],
                    3,
                    rows=peer[d],
                    chan=other[k],
                ).start()
            if d:
                remote(
                    back.at[d, pl.ds(0, 5)], returned.at[d, pl.ds(0, 5)], 2, rows=peer[d]
                ).start()
    for k in range(1, NCHAN):
        remote(spreads.at[0], spreads.at[k], 4, chan=other[k]).start()

    returned[0] = back[0]
    count_ref[...] = count
    for c in range(CH):
        mean_ref[c] = means[c]
        var_ref[c] = variances[c]

    waited = returned.at[pl.ds(0, NROW - 1), pl.ds(0, 5)]
    remote(waited, waited, 2, rows=me).wait()
    waited = partial.at[pl.ds(1, NCHAN - 1)]
    remote(waited, waited, 3, rows=me).wait()
    row = iota((8, CAP), 0)
    for d in range(NROW):
        rest = partial[1, d : d + 1] + partial[2, d : d + 1] + partial[3, d : d + 1]
        ret_ref[d] = returned[d] + jnp.where(row == 4, jnp.broadcast_to(rest, (8, CAP)), 0.0)
    waited = spreads.at[pl.ds(1, NCHAN - 1)]
    remote(waited, waited, 4, rows=me).wait()
    spread_ref[...] = (spreads[0] + spreads[1]) + (spreads[2] + spreads[3])


def last_kernel(
    ret_ref,
    rank_ref,
    brel_ref,
    mean_ref,
    var_ref,
    count_ref,
    spread_ref,
    count_out,
    mean_out,
    var_out,
    spread_out,
    dep_out,
    hot,
):
    for part in range(6):
        lo, hi = WIDE * part, min(WIDE * part + WIDE, COLS)
        take = (slice(4 * part, 4 * part + 4), slice(0, hi - lo))
        count_out[:, lo:hi] = count_ref[take].astype(jnp.int32)
        spread_out[:, lo:hi] = spread_ref[take]
        for c in range(CH):
            mean_out[c, :, lo:hi] = mean_ref[(c, *take)]
            var_out[c, :, lo:hi] = var_ref[(c, *take)]
    hot_into(hot, 0, slice(0, OBS), rows16(rank_ref[...]), CAP // 16, OBS)
    packed = ret_ref[...].reshape(NROW * 8, CAP)
    high = high_of(packed)
    pieces = jnp.concatenate([high, packed - high], axis=1).astype(BF16)
    lanes = 512
    for t in range(OBS // lanes):
        cols = slice(t * lanes, t * lanes + lanes)
        twice = jnp.concatenate([hot[:, cols], hot[:, cols]], axis=0)
        found = jnp.dot(pieces, twice, preferred_element_type=F32)
        names = jnp.broadcast_to(brel_ref[:, cols], (8, lanes))
        total = jnp.zeros((8, lanes), F32)
        for d in range(NROW):
            total = total + jnp.where(names == float(d), found[8 * d : 8 * d + 8], 0.0)
        scale = lax.rsqrt(1.0 + total[4:5] / CHAN)
        dep_out[:, cols] = total[0:4] * scale


def body(radiances, band, row_in_band, column):
    vmem = pl.BlockSpec(memory_space=pltpu.VMEM)
    shape = jax.ShapeDtypeStruct
    grid = (NCELL, WIDE)
    made = pl.pallas_call(
        comm_kernel,
        out_shape=(
            shape((NROW, 8, CAP), F32),
            shape((1, OBS), F32),
            shape((1, OBS), F32),
            shape((CH, *grid), F32),
            shape((CH, *grid), F32),
            shape(grid, F32),
            shape(grid, F32),
        ),
        in_specs=[vmem] * 4,
        out_specs=(vmem,) * 7,
        scratch_shapes=[
            pltpu.VMEM((16 * NROW, OBS), BF16),
            pltpu.VMEM((CAP, OBS), BF16),
            pltpu.VMEM((NROW, 8, CAP), F32),
            pltpu.VMEM((NROW, 8, CAP), F32),
            pltpu.VMEM((16 * NCELL + 32, 16 * CAP), BF16),
            pltpu.VMEM((WIDE, NROW * CAP), BF16),
            pltpu.VMEM((2, 16 * NCELL + 32, CAP), F32),
            pltpu.VMEM((10 * NCELL, WIDE), BF16),
            pltpu.VMEM((NROW, 8, CAP), F32),
            pltpu.VMEM((NROW, 8, CAP), F32),
            pltpu.VMEM((NCHAN, NROW, CAP), F32),
            pltpu.VMEM((NCHAN, *grid), F32),
            pltpu.SemaphoreType.DMA((5,)),
            pltpu.SemaphoreType.DMA((5,)),
            pltpu.SemaphoreType.REGULAR,
        ],
        compiler_params=pltpu.CompilerParams(collective_id=0, has_side_effects=True),
    )(
        radiances,
        band.reshape(1, OBS),
        row_in_band.reshape(1, OBS),
        column.reshape(1, OBS),
    )
    return pl.pallas_call(
        last_kernel,
        out_shape=(
            shape((4, COLS), jnp.int32),
            shape((CH, 4, COLS), F32),
            shape((CH, 4, COLS), F32),
            shape((4, COLS), F32),
            shape((CH, OBS), F32),
        ),
        in_specs=[vmem] * 7,
        out_specs=(vmem,) * 5,
        scratch_shapes=[pltpu.VMEM((CAP, OBS), BF16)],
    )(*made)


def solution(mesh):
    in_specs = (P("chan", "rows"), P("rows", None), P("rows"), P("rows"))
    out_specs = (
        P("rows", None),
        P("chan", "rows", None),
        P("chan", "rows", None),
        P("rows", None),
        P("chan", "rows"),
    )
    return jax.shard_map(body, mesh=mesh, in_specs=in_specs, out_specs=out_specs, check_vma=False)
```

```python
import functools

import jax
import jax.numpy as jnp
from jax import lax
from jax.experimental import pallas as pl
from jax.experimental.pallas import tpu as pltpu
from jax.sharding import PartitionSpec as P

CHAN = 16
COLS = 1440
NROW = 32
NCHAN = 4
CH = 4
OBS = 2048
CAP = 128
WIDE = 256
NCELL = 24
MESH = pl.DeviceIdType.MESH
F32 = jnp.float32
BF16 = jnp.bfloat16


def hops(offset):
    ring = (0, 1, 2, 1)
    return ring[offset >> 3] + ring[(offset >> 1) & 3]


NEAR = tuple(sorted(range(NROW), key=hops))
FAR = tuple(d for d in reversed(NEAR) if d)
GROUPS = (NEAR[:16], NEAR[16:])


def iota(shape, dim):
    return lax.broadcasted_iota(jnp.int32, shape, dim)


def rows16(row):
    return jnp.broadcast_to(row, (16, row.shape[1])).astype(BF16)


def count16(lanes):
    return iota((16, lanes), 0).astype(F32).astype(BF16)


def hot_into(ref, top, cols, names, blocks, lanes, first=0):
    one, zero = jnp.ones((16, lanes), BF16), jnp.zeros((16, lanes), BF16)
    steps = count16(lanes)
    for k in range(blocks):
        ref[top + 16 * k : top + 16 * k + 16, cols] = jnp.where(
            names == steps + jnp.asarray(16 * k + first, BF16), one, zero
        )


def high_of(x):
    return x.astype(BF16).astype(F32)


def spread_into_slots(radiances, bands, rib, column, left, right, rank_ref, tiles):
    lanes = OBS
    names = rows16(bands)
    hot_into(right, 0, slice(0, lanes), names, 2, lanes)
    blocks = [right[0:32, WIDE * j : WIDE * j + WIDE] for j in range(OBS // WIDE)]
    before, seen = [], jnp.zeros((32, WIDE), BF16)
    for block in blocks:
        before.append(seen)
        seen = seen + block
    stacked = jnp.concatenate(
        [jnp.concatenate(before, axis=0), jnp.concatenate(blocks, axis=0)], axis=1
    )
    ones = jnp.ones((WIDE, WIDE), BF16)
    upper = jnp.where(iota((WIDE, WIDE), 0) <= iota((WIDE, WIDE), 1), 1.0, 0.0).astype(BF16)
    prefix = jnp.dot(
        stacked, jnp.concatenate([ones, upper], axis=0), preferred_element_type=F32
    )
    ranks = []
    for j, block in enumerate(blocks):
        own = block.astype(F32) * prefix[32 * j : 32 * j + 32]
        ranks.append(jnp.sum(own, axis=0, keepdims=True) - 1.0)
    rank = jnp.concatenate(ranks, axis=1)
    rank_ref[...] = rank
    hot_into(right, 0, slice(0, lanes), rows16(rank), CAP // 16, lanes)

    row = iota((8, lanes), 0)
    both = jnp.concatenate([radiances, radiances], axis=0)
    high = high_of(both)
    middle = high_of(both - high)
    low = both - high - middle
    cell_hi = jnp.broadcast_to(((column >> 8) * 4 + rib + 1).astype(F32), (8, lanes))
    cell_lo = jnp.broadcast_to((column & 255).astype(F32), (8, lanes))
    names_of = jnp.where(row == 4, cell_hi, jnp.where(row == 5, cell_lo, 0.0))
    payload = jnp.concatenate(
        [jnp.where(row < 4, high, middle), jnp.where(row < 4, low, names_of)], axis=0
    ).astype(BF16)
    zero = jnp.zeros((16, lanes), BF16)
    for b in range(NROW):
        left[16 * b : 16 * b + 16, :] = jnp.where(names == jnp.asarray(b, BF16), payload, zero)
    placed = lax.dot_general(
        left[...], right[...], (((1,), (1,)), ((), ())), preferred_element_type=F32
    ).reshape(NROW, 16, CAP)
    upper_half, lower_half = placed[:, :8], placed[:, 8:]
    tile_row = iota((NROW, 8, CAP), 1)
    total = upper_half + pltpu.roll(upper_half, 4, 1) + lower_half
    tiles[...] = jnp.where(tile_row < 4, total, lower_half)


def comm_kernel(
    rad_hbm,
    band_hbm,
    rib_hbm,
    col_hbm,
    ret_ref,
    rank_ref,
    brel_ref,
    mean_ref,
    var_ref,
    count_ref,
    spread_ref,
    rad_ref,
    band_ref,
    rib_ref,
    col_ref,
    left,
    right,
    tiles,
    arrived,
    features,
    hot,
    sums,
    table,
    back,
    returned,
    partial,
    spreads,
    send_sem,
    recv_sem,
    ready_sem,
    load_sem,
):
    loads = [
        pltpu.make_async_copy(src, dst, load_sem.at[i])
        for i, (src, dst) in enumerate(
            ((band_hbm, band_ref), (rad_hbm, rad_ref), (rib_hbm, rib_ref), (col_hbm, col_ref))
        )
    ]
    for load in loads:
        load.start()
    me, mine = lax.axis_index("rows"), lax.axis_index("chan")
    peer = {d: lax.bitwise_xor(me, d) for d in range(NROW)}
    other = {k: lax.bitwise_xor(mine, k) for k in range(NCHAN)}
    barrier = pltpu.get_barrier_semaphore()
    for d in FAR:
        pl.semaphore_signal(barrier, 1, device_id={"rows": peer[d]}, device_id_type=MESH)
    for k in range(1, NCHAN):
        pl.semaphore_signal(barrier, 1, device_id={"chan": other[k]}, device_id_type=MESH)

    for load in loads:
        load.wait()
    bands = lax.bitwise_xor(band_ref[...], me).astype(F32)
    brel_ref[...] = bands
    spread_into_slots(
        rad_ref[...], bands, rib_ref[...], col_ref[...], left, right, rank_ref, tiles
    )
    arrived[0] = tiles[0]
    pl.semaphore_wait(barrier, NROW - 1 + NCHAN - 1)

    def remote(src, dst, which, **to):
        return pltpu.make_async_remote_copy(
            src_ref=src,
            dst_ref=dst,
            send_sem=send_sem.at[which],
            recv_sem=recv_sem.at[which],
            device_id=to,
            device_id_type=MESH,
        )

    for d in FAR:
        which = 0 if d in GROUPS[0] else 1
        remote(
            tiles.at[d, pl.ds(0, 6)], arrived.at[d, pl.ds(0, 6)], which, rows=peer[d]
        ).start()
    for k in range(1, NCHAN):
        pl.semaphore_signal(ready_sem, 1, device_id={"chan": other[k]}, device_id_type=MESH)

    for g, group in enumerate(GROUPS):
        n = len(group)
        lanes = n * CAP
        cols = slice(g * lanes, (g + 1) * lanes)
        waited = arrived.at[pl.ds(0, n - (0 in group)), pl.ds(0, 6)]
        remote(waited, waited, g, rows=me).wait()
        row = iota((8, lanes), 0)
        tile = jnp.concatenate([arrived[d] for d in group], axis=1)
        value = jnp.where(row < 4, tile, pltpu.roll(tile, 4, 0))
        square = value * value
        value_hi, square_hi = high_of(value), high_of(square)
        feature = jnp.concatenate(
            [
                jnp.where(row < 4, value_hi, value - value_hi),
                jnp.where(row < 4, square_hi, square - square_hi),
            ],
            axis=0,
        ).astype(BF16)
        cell_hi = rows16(jnp.concatenate([arrived[d, 4:5] for d in group], axis=1))
        cell_lo = rows16(jnp.concatenate([arrived[d, 5:6] for d in group], axis=1))
        zero = jnp.zeros((16, lanes), BF16)
        for a in range(NCELL):
            features[16 * a : 16 * a + 16, :] = jnp.where(
                cell_hi == jnp.asarray(a + 1, BF16), feature, zero
            )
        hot_into(features, 16 * NCELL, slice(0, lanes), cell_hi, 2, lanes, first=1)
        hot_into(hot, 0, cols, cell_lo, WIDE // 16, lanes)
        part = lax.dot_general(
            features[...], hot[:, cols], (((1,), (1,)), ((), ())), preferred_element_type=F32
        )
        for half in range(2):
            piece = part[:, CAP * half : CAP * half + CAP]
            if g == 0:
                sums[half] = piece
            else:
                sums[half] += piece

    def both_halves(pick):
        return jnp.concatenate([sums[half, pick, :] for half in range(2)], axis=1)

    count = both_halves(slice(16 * NCELL, 16 * NCELL + NCELL))
    inverse = 1.0 / jnp.maximum(count, 1.0)
    means, variances = [], []
    for c in range(CH):
        pick = lambda f: both_halves(pl.ds(f, NCELL, stride=16))
        mean = (pick(c) + pick(c + 4)) * inverse
        var = jnp.maximum((pick(c + 8) + pick(c + 12)) * inverse - mean * mean, 0.0)
        means.append(mean)
        variances.append(var)
    own_spread = (variances[0] + variances[1]) + (variances[2] + variances[3])
    spreads[0] = own_spread
    fields = means + [own_spread]
    highs = [high_of(x) for x in fields]
    lows = [x - h for x, h in zip(fields, highs)]
    table[...] = jnp.concatenate(highs + lows, axis=0).astype(BF16)

    nfield = len(fields)
    order = [d for group in GROUPS for d in group]
    turn = 4
    for t in reversed(range(NROW // turn)):
        group = order[turn * t : turn * t + turn]
        lanes = turn * CAP
        found = jnp.dot(
            table[...], hot[:, lanes * t : lanes * t + lanes], preferred_element_type=F32
        ).reshape(2 * nfield, NCELL, lanes)
        found = found[:nfield] + found[nfield:]
        cell_hi = jnp.concatenate([arrived[d, 4:5] for d in group], axis=1)
        here = jnp.broadcast_to(cell_hi, (NCELL, lanes)) == (iota((NCELL, lanes), 0) + 1).astype(F32)
        row = iota((8, lanes), 0)
        looked = jnp.zeros((8, lanes), F32)
        for f in range(nfield):
            only = jnp.where(here, found[f], 0.0)
            only = only[0:8] + only[8:16] + only[16:24]
            only = only + pltpu.roll(only, 4, 0)
            only = only + pltpu.roll(only, 2, 0)
            only = only + pltpu.roll(only, 1, 0)
            looked = jnp.where(row == f, only, looked)
        tile = jnp.concatenate([arrived[d] for d in group], axis=1)
        tile = jnp.where(row < 4, tile - looked, looked)
        for i, d in enumerate(group):
            back[d] = tile[:, CAP * i : CAP * i + CAP]
        if t == NROW // turn - 1:
            pl.semaphore_wait(ready_sem, NCHAN - 1)
        for d in reversed(group):
            for k in (2, 1, 3):
                remote(
                    back.at[d, pl.ds(4, 1)],
                    partial.at[k, pl.ds(d, 1)],
                    3,
                    rows=peer[d],
                    chan=other[k],
                ).start()
            if d:
                remote(
                    back.at[d, pl.ds(0, 5)], returned.at[d, pl.ds(0, 5)], 2, rows=peer[d]
                ).start()
    for k in range(1, NCHAN):
        remote(spreads.at[0], spreads.at[k], 4, chan=other[k]).start()

    returned[0] = back[0]
    count_ref[...] = count
    for c in range(CH):
        mean_ref[c] = means[c]
        var_ref[c] = variances[c]

    waited = returned.at[pl.ds(0, NROW - 1), pl.ds(0, 5)]
    remote(waited, waited, 2, rows=me).wait()
    waited = partial.at[pl.ds(1, NCHAN - 1)]
    remote(waited, waited, 3, rows=me).wait()
    row = iota((8, CAP), 0)
    for d in range(NROW):
        rest = partial[1, d : d + 1] + partial[2, d : d + 1] + partial[3, d : d + 1]
        ret_ref[d] = returned[d] + jnp.where(row == 4, jnp.broadcast_to(rest, (8, CAP)), 0.0)
    waited = spreads.at[pl.ds(1, NCHAN - 1)]
    remote(waited, waited, 4, rows=me).wait()
    spread_ref[...] = (spreads[0] + spreads[1]) + (spreads[2] + spreads[3])


def last_kernel(
    ret_ref,
    rank_ref,
    brel_ref,
    mean_ref,
    var_ref,
    count_ref,
    spread_ref,
    count_out,
    mean_out,
    var_out,
    spread_out,
    dep_out,
    hot,
):
    for part in range(6):
        lo, hi = WIDE * part, min(WIDE * part + WIDE, COLS)
        take = (slice(4 * part, 4 * part + 4), slice(0, hi - lo))
        count_out[:, lo:hi] = count_ref[take].astype(jnp.int32)
        spread_out[:, lo:hi] = spread_ref[take]
        for c in range(CH):
            mean_out[c, :, lo:hi] = mean_ref[(c, *take)]
            var_out[c, :, lo:hi] = var_ref[(c, *take)]
    hot_into(hot, 0, slice(0, OBS), rows16(rank_ref[...]), CAP // 16, OBS)
    packed = ret_ref[...].reshape(NROW * 8, CAP)
    high = high_of(packed)
    pieces = jnp.concatenate([high, packed - high], axis=1).astype(BF16)
    lanes = 512
    for t in range(OBS // lanes):
        cols = slice(t * lanes, t * lanes + lanes)
        twice = jnp.concatenate([hot[:, cols], hot[:, cols]], axis=0)
        found = jnp.dot(pieces, twice, preferred_element_type=F32)
        names = jnp.broadcast_to(brel_ref[:, cols], (8, lanes))
        total = jnp.zeros((8, lanes), F32)
        for d in range(NROW):
            total = total + jnp.where(names == float(d), found[8 * d : 8 * d + 8], 0.0)
        scale = lax.rsqrt(1.0 + total[4:5] / CHAN)
        dep_out[:, cols] = total[0:4] * scale


def body(radiances, band, row_in_band, column):
    vmem = pl.BlockSpec(memory_space=pltpu.VMEM)
    shape = jax.ShapeDtypeStruct
    grid = (NCELL, WIDE)
    made = pl.pallas_call(
        comm_kernel,
        out_shape=(
            shape((NROW, 8, CAP), F32),
            shape((1, OBS), F32),
            shape((1, OBS), F32),
            shape((CH, *grid), F32),
            shape((CH, *grid), F32),
            shape(grid, F32),
            shape(grid, F32),
        ),
        in_specs=[pl.BlockSpec(memory_space=pltpu.HBM)] * 4,
        out_specs=(vmem,) * 7,
        scratch_shapes=[
            pltpu.VMEM((CH, OBS), F32),
            pltpu.VMEM((1, OBS), jnp.int32),
            pltpu.VMEM((1, OBS), jnp.int32),
            pltpu.VMEM((1, OBS), jnp.int32),
            pltpu.VMEM((16 * NROW, OBS), BF16),
            pltpu.VMEM((CAP, OBS), BF16),
            pltpu.VMEM((NROW, 8, CAP), F32),
            pltpu.VMEM((NROW, 8, CAP), F32),
            pltpu.VMEM((16 * NCELL + 32, 16 * CAP), BF16),
            pltpu.VMEM((WIDE, NROW * CAP), BF16),
            pltpu.VMEM((2, 16 * NCELL + 32, CAP), F32),
            pltpu.VMEM((10 * NCELL, WIDE), BF16),
            pltpu.VMEM((NROW, 8, CAP), F32),
            pltpu.VMEM((NROW, 8, CAP), F32),
            pltpu.VMEM((NCHAN, NROW, CAP), F32),
            pltpu.VMEM((NCHAN, *grid), F32),
            pltpu.SemaphoreType.DMA((5,)),
            pltpu.SemaphoreType.DMA((5,)),
            pltpu.SemaphoreType.REGULAR,
            pltpu.SemaphoreType.DMA((4,)),
        ],
        compiler_params=pltpu.CompilerParams(
            collective_id=0, has_side_effects=True, vmem_limit_bytes=24 << 20
        ),
    )(
        *(
            pltpu.with_memory_space_constraint(x, pltpu.HBM)
            for x in (
                radiances,
                band.reshape(1, OBS),
                row_in_band.reshape(1, OBS),
                column.reshape(1, OBS),
            )
        )
    )
    return pl.pallas_call(
        last_kernel,
        out_shape=(
            shape((4, COLS), jnp.int32),
            shape((CH, 4, COLS), F32),
            shape((CH, 4, COLS), F32),
            shape((4, COLS), F32),
            shape((CH, OBS), F32),
        ),
        in_specs=[vmem] * 7,
        out_specs=(vmem,) * 5,
        scratch_shapes=[pltpu.VMEM((CAP, OBS), BF16)],
        compiler_params=pltpu.CompilerParams(vmem_limit_bytes=16 << 20),
    )(*made)


def solution(mesh):
    in_specs = (P("chan", "rows"), P("rows", None), P("rows"), P("rows"))
    out_specs = (
        P("rows", None),
        P("chan", "rows", None),
        P("chan", "rows", None),
        P("rows", None),
        P("chan", "rows"),
    )
    return jax.shard_map(body, mesh=mesh, in_specs=in_specs, out_specs=out_specs, check_vma=False)
```

```python
import functools

import jax
import jax.numpy as jnp
from jax import lax
from jax.experimental import pallas as pl
from jax.experimental.pallas import tpu as pltpu
from jax.sharding import PartitionSpec as P

CHAN = 16
COLS = 1440
NROW = 32
NCHAN = 4
CH = 4
OBS = 2048
CAP = 128
WIDE = 256
NCELL = 24
MESH = pl.DeviceIdType.MESH
F32 = jnp.float32
BF16 = jnp.bfloat16


def hops(offset):
    ring = (0, 1, 2, 1)
    return ring[offset >> 3] + ring[(offset >> 1) & 3]


NEAR = tuple(sorted(range(NROW), key=hops))
FAR = tuple(d for d in reversed(NEAR) if d)
GROUPS = (NEAR[0:8], NEAR[8:20], NEAR[20:32])
BACK = (NEAR,)
FIELDS = 16


def iota(shape, dim):
    return lax.broadcasted_iota(jnp.int32, shape, dim)


def rows16(row):
    return jnp.broadcast_to(row, (16, row.shape[1])).astype(BF16)


def count16(lanes):
    return iota((16, lanes), 0).astype(F32).astype(BF16)


def hot_into(ref, top, cols, names, blocks, lanes, first=0):
    one, zero = jnp.ones((16, lanes), BF16), jnp.zeros((16, lanes), BF16)
    steps = count16(lanes)
    for k in range(blocks):
        ref[top + 16 * k : top + 16 * k + 16, cols] = jnp.where(
            names == steps + jnp.asarray(16 * k + first, BF16), one, zero
        )


def high_of(x):
    return x.astype(BF16).astype(F32)


def spread_into_slots(radiances, bands, rib, column, left, right, tiles):
    lanes = OBS
    names = rows16(bands)
    hot_into(right, 0, slice(0, lanes), names, 2, lanes)
    blocks = [right[0:32, WIDE * j : WIDE * j + WIDE] for j in range(OBS // WIDE)]
    before, seen = [], jnp.zeros((32, WIDE), BF16)
    for block in blocks:
        before.append(seen)
        seen = seen + block
    stacked = jnp.concatenate(
        [jnp.concatenate(before, axis=0), jnp.concatenate(blocks, axis=0)], axis=1
    )
    ones = jnp.ones((WIDE, WIDE), BF16)
    upper = jnp.where(iota((WIDE, WIDE), 0) <= iota((WIDE, WIDE), 1), 1.0, 0.0).astype(BF16)
    prefix = jnp.dot(
        stacked, jnp.concatenate([ones, upper], axis=0), preferred_element_type=F32
    )
    ranks = []
    for j, block in enumerate(blocks):
        own = block.astype(F32) * prefix[32 * j : 32 * j + 32]
        ranks.append(jnp.sum(own, axis=0, keepdims=True) - 1.0)
    rank = jnp.concatenate(ranks, axis=1)
    hot_into(right, 0, slice(0, lanes), rows16(rank), CAP // 16, lanes)

    row = iota((8, lanes), 0)
    both = jnp.concatenate([radiances, radiances], axis=0)
    high = high_of(both)
    middle = high_of(both - high)
    low = both - high - middle
    cell_hi = jnp.broadcast_to(((column >> 8) * 4 + rib + 1).astype(F32), (8, lanes))
    cell_lo = jnp.broadcast_to((column & 255).astype(F32), (8, lanes))
    names_of = jnp.where(row == 4, cell_hi, jnp.where(row == 5, cell_lo, 0.0))
    payload = jnp.concatenate(
        [jnp.where(row < 4, high, middle), jnp.where(row < 4, low, names_of)], axis=0
    ).astype(BF16)
    zero = jnp.zeros((16, lanes), BF16)
    for b in range(NROW):
        left[16 * b : 16 * b + 16, 0:OBS] = jnp.where(names == jnp.asarray(b, BF16), payload, zero)
    placed = lax.dot_general(
        left[:, 0:OBS], right[...], (((1,), (1,)), ((), ())), preferred_element_type=F32
    ).reshape(NROW, 16, CAP)
    upper_half, lower_half = placed[:, :8], placed[:, 8:]
    tile_row = iota((NROW, 8, CAP), 1)
    total = upper_half + pltpu.roll(upper_half, 4, 1) + lower_half
    tiles[...] = jnp.where(
        tile_row < 4, total, lower_half * 256.0 + pltpu.roll(lower_half, 7, 1)
    )


def feature_rows(ref, f1, f2, lanes):
    first = jnp.broadcast_to(ref[f1 : f1 + 1, 0:lanes], (8, lanes))
    second = jnp.broadcast_to(ref[f2 : f2 + 1, 0:lanes], (8, lanes))
    return [
        jnp.concatenate(pair, axis=0).astype(BF16)
        for pair in ((first, first), (first, second), (second, second))
    ]


def accumulate(arrived, group, rows, left, hot, cols):
    lanes = len(group) * CAP
    row = iota((8, lanes), 0)
    tile = jnp.concatenate([arrived[d] for d in group], axis=1)
    code = jnp.concatenate(
        [jnp.broadcast_to(arrived[d, 4:5], (8, CAP)) for d in group], axis=1
    )
    value = jnp.where(row < 4, tile, pltpu.roll(tile, 4, 0))
    square = value * value
    value_hi, square_hi = high_of(value), high_of(square)
    rows[0:8, 0:lanes] = jnp.where(row < 4, value_hi, value - value_hi)
    rows[8:16, 0:lanes] = jnp.where(row < 4, square_hi, square - square_hi)
    cell_hi = jnp.floor(code * (1.0 / 256.0))
    cell_lo = code - 256.0 * cell_hi
    hi16 = jnp.concatenate([cell_hi, cell_hi], axis=0).astype(BF16)
    lo16 = jnp.concatenate([cell_lo, cell_lo], axis=0).astype(BF16)
    step = iota((16, lanes), 0)
    names = (step + 1, jnp.where(step < 8, step + 17, step - 7), step + 9)
    masks = [hi16 == n.astype(F32).astype(BF16) for n in names]
    zero = jnp.zeros((16, lanes), BF16)
    for pair in range(FIELDS // 2):
        for i, source in enumerate(feature_rows(rows, 2 * pair, 2 * pair + 1, lanes)):
            at = 48 * pair + 16 * i
            left[at : at + 16, 0:lanes] = jnp.where(masks[i], source, zero)
    hot_into(left, FIELDS * NCELL, slice(0, lanes), hi16, 2, lanes, first=1)
    hot_into(hot, 0, cols, lo16, WIDE // 16, lanes)
    return lax.dot_general(
        left[0 : FIELDS * NCELL + 32, 0:lanes],
        hot[:, cols],
        (((1,), (1,)), ((), ())),
        preferred_element_type=F32,
    )


def comm_kernel(
    rad_hbm,
    band_hbm,
    rib_hbm,
    col_hbm,
    count_out,
    mean_out,
    var_out,
    spread_out,
    ret_ref,
    right,
    brel,
    rad_ref,
    band_ref,
    rib_ref,
    col_ref,
    left,
    tiles,
    arrived,
    rows,
    hot,
    sums,
    table,
    back,
    returned,
    partial,
    spreads,
    send_sem,
    recv_sem,
    ready_sem,
    load_sem,
):
    loads = [
        pltpu.make_async_copy(src, dst, load_sem.at[i])
        for i, (src, dst) in enumerate(
            ((band_hbm, band_ref), (rad_hbm, rad_ref), (rib_hbm, rib_ref), (col_hbm, col_ref))
        )
    ]
    for load in loads:
        load.start()
    me, mine = lax.axis_index("rows"), lax.axis_index("chan")
    peer = {d: lax.bitwise_xor(me, d) for d in range(NROW)}
    other = {k: lax.bitwise_xor(mine, k) for k in range(NCHAN)}
    barrier = pltpu.get_barrier_semaphore()
    for d in FAR:
        pl.semaphore_signal(barrier, 1, device_id={"rows": peer[d]}, device_id_type=MESH)
    for k in range(1, NCHAN):
        pl.semaphore_signal(barrier, 1, device_id={"chan": other[k]}, device_id_type=MESH)

    for load in loads:
        load.wait()
    bands = lax.bitwise_xor(band_ref[...], me).astype(F32)
    brel[...] = bands
    spread_into_slots(rad_ref[...], bands, rib_ref[...], col_ref[...], left, right, tiles)
    arrived[0] = tiles[0]
    pl.semaphore_wait(barrier, NROW - 1 + NCHAN - 1)

    def remote(src, dst, which, **to):
        return pltpu.make_async_remote_copy(
            src_ref=src,
            dst_ref=dst,
            send_sem=send_sem.at[which],
            recv_sem=recv_sem.at[which],
            device_id=to,
            device_id_type=MESH,
        )

    def group_of(d, groups):
        return [d in group for group in groups].index(True)

    def wait_tiles(buffer, group, which):
        part = buffer.at[pl.ds(0, len(group) - (0 in group)), pl.ds(0, 5)]
        remote(part, part, which, rows=me).wait()

    first_back = len(GROUPS)
    first_part = first_back + len(BACK)
    grid_sem = first_part + len(BACK)

    for d in FAR:
        remote(
            tiles.at[d, pl.ds(0, 5)],
            arrived.at[d, pl.ds(0, 5)],
            group_of(d, GROUPS),
            rows=peer[d],
        ).start()
    for k in range(1, NCHAN):
        pl.semaphore_signal(ready_sem, 1, device_id={"chan": other[k]}, device_id_type=MESH)

    start = 0
    for g, group in enumerate(GROUPS):
        if len(group) > (0 in group):
            wait_tiles(arrived, group, g)
        cols = slice(start, start + len(group) * CAP)
        part = accumulate(arrived, group, rows, left, hot, cols)
        start = cols.stop
        if g == 0:
            sums[...] = part
        elif g < len(GROUPS) - 1:
            sums[...] += part

    def field(f):
        at = slice(NCELL * f, NCELL * f + NCELL)
        return part[at] + sums[at]

    count = field(FIELDS)
    inverse = 1.0 / jnp.maximum(count, 1.0)
    means, variances = [], []
    for c in range(CH):
        mean = (field(c) + field(c + 4)) * inverse
        var = jnp.maximum((field(c + 8) + field(c + 12)) * inverse - mean * mean, 0.0)
        means.append(mean)
        variances.append(var)
    own_spread = (variances[0] + variances[1]) + (variances[2] + variances[3])
    spreads[0] = own_spread
    fields = means + [own_spread]
    highs = [high_of(x) for x in fields]
    lows = [x - h for x, h in zip(fields, highs)]
    table[...] = jnp.concatenate(highs + lows, axis=0).astype(BF16)

    nfield = len(fields)
    order = [d for group in GROUPS for d in group]
    turn = 4
    for t in reversed(range(NROW // turn)):
        group = order[turn * t : turn * t + turn]
        lanes = turn * CAP
        looks = jnp.dot(
            table[...], hot[:, lanes * t : lanes * t + lanes], preferred_element_type=F32
        ).reshape(2 * nfield, NCELL, lanes)
        looks = looks[:nfield] + looks[nfield:]
        code = jnp.concatenate(
            [jnp.broadcast_to(arrived[d, 4:5], (8, CAP)) for d in group], axis=1
        )
        cell_hi = jnp.floor(code * (1.0 / 256.0))
        row = iota((8, lanes), 0)
        here = [cell_hi == (row + (8 * i + 1)).astype(F32) for i in range(NCELL // 8)]
        looked = jnp.zeros((8, lanes), F32)
        for f in range(nfield):
            only = jnp.where(here[0], looks[f, 0:8], 0.0)
            for i in range(1, NCELL // 8):
                only = only + jnp.where(here[i], looks[f, 8 * i : 8 * i + 8], 0.0)
            only = only + pltpu.roll(only, 4, 0)
            only = only + pltpu.roll(only, 2, 0)
            only = only + pltpu.roll(only, 1, 0)
            looked = jnp.where(row == f, only, looked)
        tile = jnp.concatenate([arrived[d] for d in group], axis=1)
        tile = jnp.where(row < 4, tile - looked, looked)
        for i, d in enumerate(group):
            back[d] = tile[:, CAP * i : CAP * i + CAP]
        if t == NROW // turn - 1:
            pl.semaphore_wait(ready_sem, NCHAN - 1)
        for d in reversed(group):
            g = group_of(d, BACK)
            for k in (2, 1, 3):
                remote(
                    back.at[d, pl.ds(4, 1)],
                    partial.at[pl.ds((k - 1) * NROW + d, 1)],
                    first_part + g,
                    rows=peer[d],
                    chan=other[k],
                ).start()
            if d:
                remote(
                    back.at[d, pl.ds(0, 5)],
                    returned.at[d, pl.ds(0, 5)],
                    first_back + g,
                    rows=peer[d],
                ).start()

    for k in range(1, NCHAN):
        remote(spreads.at[0], spreads.at[k], grid_sem, chan=other[k]).start()

    def to_rows(part, out, grid):
        lo, hi = WIDE * part, min(WIDE * part + WIDE, COLS)
        out[:, lo:hi] = grid[4 * part : 4 * part + 4, 0 : hi - lo].astype(out.dtype)

    returned[0] = back[0]
    for part in range(6):
        to_rows(part, count_out, count)
        for c in range(CH):
            to_rows(part, mean_out.at[c], means[c])
            to_rows(part, var_out.at[c], variances[c])

    wait_tiles(returned, NEAR, first_back)
    waited = spreads.at[pl.ds(1, NCHAN - 1)]
    remote(waited, waited, grid_sem, rows=me).wait()
    spread = (spreads[0] + spreads[1]) + (spreads[2] + spreads[3])
    for part in range(6):
        to_rows(part, spread_out, spread)
    remote(partial, partial, first_part, rows=me).wait()
    row = iota((8, CAP), 0)
    for d in range(NROW):
        at = [slice(k * NROW + d, k * NROW + d + 1) for k in range(NCHAN - 1)]
        rest = partial[at[0]] + partial[at[1]] + partial[at[2]]
        ret_ref[d] = returned[d] + jnp.where(row == 4, jnp.broadcast_to(rest, (8, CAP)), 0.0)


def last_kernel(
    count_ref,
    mean_ref,
    var_ref,
    spread_ref,
    ret_ref,
    right,
    brel,
    count_hbm,
    mean_hbm,
    var_hbm,
    spread_hbm,
    dep_hbm,
    dep_ref,
    sem,
):
    pairs = (
        (mean_ref, mean_hbm),
        (var_ref, var_hbm),
        (count_ref, count_hbm),
        (spread_ref, spread_hbm),
        (dep_ref, dep_hbm),
    )
    copies = [
        pltpu.make_async_copy(src, dst, sem.at[i]) for i, (src, dst) in enumerate(pairs)
    ]
    for copy in copies[:4]:
        copy.start()
    packed = ret_ref[...].reshape(NROW * 8, CAP)
    high = high_of(packed)
    pieces = jnp.concatenate([high, packed - high], axis=1).astype(BF16)
    lanes = 512
    for t in range(OBS // lanes):
        cols = slice(t * lanes, t * lanes + lanes)
        twice = jnp.concatenate([right[:, cols], right[:, cols]], axis=0)
        found = jnp.dot(pieces, twice, preferred_element_type=F32)
        names = jnp.broadcast_to(brel[:, cols], (8, lanes))
        total = jnp.zeros((8, lanes), F32)
        for d in range(NROW):
            total = total + jnp.where(names == float(d), found[8 * d : 8 * d + 8], 0.0)
        dep_ref[:, cols] = total[0:4] * lax.rsqrt(1.0 + total[4:5] / CHAN)
    copies[4].start()
    for copy in copies:
        copy.wait()


def body(radiances, band, row_in_band, column):
    vmem = pl.BlockSpec(memory_space=pltpu.VMEM)
    hbm = pl.BlockSpec(memory_space=pltpu.HBM)
    shape = jax.ShapeDtypeStruct
    grid = (NCELL, WIDE)
    outs = (
        shape((4, COLS), jnp.int32),
        shape((CH, 4, COLS), F32),
        shape((CH, 4, COLS), F32),
        shape((4, COLS), F32),
        shape((CH, OBS), F32),
    )
    between = (
        *outs[:4],
        shape((NROW, 8, CAP), F32),
        shape((CAP, OBS), BF16),
        shape((1, OBS), F32),
    )
    nsem = len(GROUPS) + 2 * len(BACK) + 1
    operands = (
        radiances,
        band.reshape(1, OBS),
        row_in_band.reshape(1, OBS),
        column.reshape(1, OBS),
    )
    made = pl.pallas_call(
        comm_kernel,
        out_shape=between,
        in_specs=[hbm] * 4,
        out_specs=(vmem,) * 7,
        scratch_shapes=[
            pltpu.VMEM((CH, OBS), F32),
            pltpu.VMEM((1, OBS), jnp.int32),
            pltpu.VMEM((1, OBS), jnp.int32),
            pltpu.VMEM((1, OBS), jnp.int32),
            pltpu.VMEM((16 * NROW, 22 * CAP), BF16),
            pltpu.VMEM((NROW, 8, CAP), F32),
            pltpu.VMEM((NROW, 8, CAP), F32),
            pltpu.VMEM((FIELDS, 22 * CAP), F32),
            pltpu.VMEM((WIDE, NROW * CAP), BF16),
            pltpu.VMEM((FIELDS * NCELL + 32, WIDE), F32),
            pltpu.VMEM((10 * NCELL, WIDE), BF16),
            pltpu.VMEM((NROW, 8, CAP), F32),
            pltpu.VMEM((NROW, 8, CAP), F32),
            pltpu.VMEM(((NCHAN - 1) * NROW, CAP), F32),
            pltpu.VMEM((NCHAN, *grid), F32),
            pltpu.SemaphoreType.DMA((nsem,)),
            pltpu.SemaphoreType.DMA((nsem,)),
            pltpu.SemaphoreType.REGULAR,
            pltpu.SemaphoreType.DMA((4,)),
        ],
        compiler_params=pltpu.CompilerParams(
            collective_id=0, has_side_effects=True, vmem_limit_bytes=24 << 20
        ),
    )(*(pltpu.with_memory_space_constraint(x, pltpu.HBM) for x in operands))
    return pl.pallas_call(
        last_kernel,
        out_shape=outs,
        in_specs=[vmem] * 7,
        out_specs=(hbm,) * 5,
        scratch_shapes=[pltpu.VMEM((CH, OBS), F32), pltpu.SemaphoreType.DMA((5,))],
        compiler_params=pltpu.CompilerParams(vmem_limit_bytes=16 << 20),
    )(*made)


def solution(mesh):
    in_specs = (P("chan", "rows"), P("rows", None), P("rows"), P("rows"))
    out_specs = (
        P("rows", None),
        P("chan", "rows", None),
        P("chan", "rows", None),
        P("rows", None),
        P("chan", "rows"),
    )
    return jax.shard_map(body, mesh=mesh, in_specs=in_specs, out_specs=out_specs, check_vma=False)
```

```python
import functools

import jax
import jax.numpy as jnp
from jax import lax
from jax.experimental import pallas as pl
from jax.experimental.pallas import tpu as pltpu
from jax.sharding import PartitionSpec as P

CHAN = 16
COLS = 1440
NROW = 32
NCHAN = 4
CH = 4
OBS = 2048
CAP = 128
WIDE = 256
NCELL = 24
MESH = pl.DeviceIdType.MESH
F32 = jnp.float32
BF16 = jnp.bfloat16


def hops(offset):
    ring = (0, 1, 2, 1)
    return ring[offset >> 3] + ring[(offset >> 1) & 3]


NEAR = tuple(sorted(range(NROW), key=hops))
FAR = tuple(d for d in reversed(NEAR) if d)
GROUPS = (NEAR[0:8], NEAR[8:20], NEAR[20:32])
BACK = (NEAR,)
FIELDS = 16


def iota(shape, dim):
    return lax.broadcasted_iota(jnp.int32, shape, dim)


def rows16(row):
    return jnp.broadcast_to(row, (16, row.shape[1])).astype(BF16)


def count16(lanes):
    return iota((16, lanes), 0).astype(F32).astype(BF16)


def hot_into(ref, top, cols, names, blocks, lanes, first=0):
    one, zero = jnp.ones((16, lanes), BF16), jnp.zeros((16, lanes), BF16)
    steps = count16(lanes)
    for k in range(blocks):
        ref[top + 16 * k : top + 16 * k + 16, cols] = jnp.where(
            names == steps + jnp.asarray(16 * k + first, BF16), one, zero
        )


def high_of(x):
    return x.astype(BF16).astype(F32)


def spread_into_slots(radiances, bands, rib, column, left, right, rank_ref, tiles):
    lanes = OBS
    names = rows16(bands)
    hot_into(right, 0, slice(0, lanes), names, 2, lanes)
    blocks = [right[0:32, WIDE * j : WIDE * j + WIDE] for j in range(OBS // WIDE)]
    before, seen = [], jnp.zeros((32, WIDE), BF16)
    for block in blocks:
        before.append(seen)
        seen = seen + block
    stacked = jnp.concatenate(
        [jnp.concatenate(before, axis=0), jnp.concatenate(blocks, axis=0)], axis=1
    )
    ones = jnp.ones((WIDE, WIDE), BF16)
    upper = jnp.where(iota((WIDE, WIDE), 0) <= iota((WIDE, WIDE), 1), 1.0, 0.0).astype(BF16)
    prefix = jnp.dot(
        stacked, jnp.concatenate([ones, upper], axis=0), preferred_element_type=F32
    )
    ranks = []
    for j, block in enumerate(blocks):
        own = block.astype(F32) * prefix[32 * j : 32 * j + 32]
        ranks.append(jnp.sum(own, axis=0, keepdims=True) - 1.0)
    rank = jnp.concatenate(ranks, axis=1)
    rank_ref[...] = rank
    hot_into(right, 0, slice(0, lanes), rows16(rank), CAP // 16, lanes)

    row = iota((8, lanes), 0)
    both = jnp.concatenate([radiances, radiances], axis=0)
    high = high_of(both)
    middle = high_of(both - high)
    low = both - high - middle
    cell_hi = jnp.broadcast_to(((column >> 8) * 4 + rib + 1).astype(F32), (8, lanes))
    cell_lo = jnp.broadcast_to((column & 255).astype(F32), (8, lanes))
    names_of = jnp.where(row == 4, cell_hi, jnp.where(row == 5, cell_lo, 0.0))
    payload = jnp.concatenate(
        [jnp.where(row < 4, high, middle), jnp.where(row < 4, low, names_of)], axis=0
    ).astype(BF16)
    zero = jnp.zeros((16, lanes), BF16)
    for b in range(NROW):
        left[16 * b : 16 * b + 16, :] = jnp.where(names == jnp.asarray(b, BF16), payload, zero)
    placed = lax.dot_general(
        left[...], right[...], (((1,), (1,)), ((), ())), preferred_element_type=F32
    ).reshape(NROW, 16, CAP)
    upper_half, lower_half = placed[:, :8], placed[:, 8:]
    tile_row = iota((NROW, 8, CAP), 1)
    total = upper_half + pltpu.roll(upper_half, 4, 1) + lower_half
    tiles[...] = jnp.where(
        tile_row < 4, total, lower_half * 256.0 + pltpu.roll(lower_half, 7, 1)
    )


def feature_rows(ref, f1, f2, lanes):
    first = jnp.broadcast_to(ref[f1 : f1 + 1, 0:lanes], (8, lanes))
    second = jnp.broadcast_to(ref[f2 : f2 + 1, 0:lanes], (8, lanes))
    return [
        jnp.concatenate(pair, axis=0).astype(BF16)
        for pair in ((first, first), (first, second), (second, second))
    ]


def accumulate(arrived, group, rows, left, hot, cols):
    lanes = len(group) * CAP
    row = iota((8, lanes), 0)
    tile = jnp.concatenate([arrived[d] for d in group], axis=1)
    code = jnp.concatenate(
        [jnp.broadcast_to(arrived[d, 4:5], (8, CAP)) for d in group], axis=1
    )
    value = jnp.where(row < 4, tile, pltpu.roll(tile, 4, 0))
    square = value * value
    value_hi, square_hi = high_of(value), high_of(square)
    rows[0:8, 0:lanes] = jnp.where(row < 4, value_hi, value - value_hi)
    rows[8:16, 0:lanes] = jnp.where(row < 4, square_hi, square - square_hi)
    cell_hi = jnp.floor(code * (1.0 / 256.0))
    cell_lo = code - 256.0 * cell_hi
    hi16 = jnp.concatenate([cell_hi, cell_hi], axis=0).astype(BF16)
    lo16 = jnp.concatenate([cell_lo, cell_lo], axis=0).astype(BF16)
    step = iota((16, lanes), 0)
    names = (step + 1, jnp.where(step < 8, step + 17, step - 7), step + 9)
    masks = [hi16 == n.astype(F32).astype(BF16) for n in names]
    zero = jnp.zeros((16, lanes), BF16)
    for pair in range(FIELDS // 2):
        for i, source in enumerate(feature_rows(rows, 2 * pair, 2 * pair + 1, lanes)):
            at = 48 * pair + 16 * i
            left[at : at + 16, 0:lanes] = jnp.where(masks[i], source, zero)
    hot_into(left, FIELDS * NCELL, slice(0, lanes), hi16, 2, lanes, first=1)
    hot_into(hot, 0, cols, lo16, WIDE // 16, lanes)
    return lax.dot_general(
        left[0 : FIELDS * NCELL + 32, 0:lanes],
        hot[:, cols],
        (((1,), (1,)), ((), ())),
        preferred_element_type=F32,
    )


def comm_kernel(
    rad_hbm,
    band_hbm,
    rib_hbm,
    col_hbm,
    count_out,
    mean_out,
    var_out,
    spread_out,
    shifted_ref,
    slots_ref,
    rank_ref,
    brel,
    rad_ref,
    band_ref,
    rib_ref,
    col_ref,
    left,
    right,
    tiles,
    arrived,
    rows,
    hot,
    sums,
    table,
    back,
    returned,
    partial,
    spreads,
    send_sem,
    recv_sem,
    ready_sem,
    load_sem,
):
    loads = [
        pltpu.make_async_copy(src, dst, load_sem.at[i])
        for i, (src, dst) in enumerate(
            ((band_hbm, band_ref), (rad_hbm, rad_ref), (rib_hbm, rib_ref), (col_hbm, col_ref))
        )
    ]
    for load in loads:
        load.start()
    me, mine = lax.axis_index("rows"), lax.axis_index("chan")
    peer = {d: lax.bitwise_xor(me, d) for d in range(NROW)}
    other = {k: lax.bitwise_xor(mine, k) for k in range(NCHAN)}
    barrier = pltpu.get_barrier_semaphore()
    for d in FAR:
        pl.semaphore_signal(barrier, 1, device_id={"rows": peer[d]}, device_id_type=MESH)
    for k in range(1, NCHAN):
        pl.semaphore_signal(barrier, 1, device_id={"chan": other[k]}, device_id_type=MESH)

    for load in loads:
        load.wait()
    bands = lax.bitwise_xor(band_ref[...], me).astype(F32)
    brel[...] = bands
    spread_into_slots(
        rad_ref[...], bands, rib_ref[...], col_ref[...], left, right, rank_ref, tiles
    )
    arrived[0] = tiles[0]
    pl.semaphore_wait(barrier, NROW - 1 + NCHAN - 1)

    def remote(src, dst, which, **to):
        return pltpu.make_async_remote_copy(
            src_ref=src,
            dst_ref=dst,
            send_sem=send_sem.at[which],
            recv_sem=recv_sem.at[which],
            device_id=to,
            device_id_type=MESH,
        )

    def group_of(d, groups):
        return [d in group for group in groups].index(True)

    def wait_tiles(buffer, group, which):
        part = buffer.at[pl.ds(0, len(group) - (0 in group)), pl.ds(0, 5)]
        remote(part, part, which, rows=me).wait()

    first_back = len(GROUPS)
    first_part = first_back + len(BACK)
    grid_sem = first_part + len(BACK)

    for d in FAR:
        remote(
            tiles.at[d, pl.ds(0, 5)],
            arrived.at[d, pl.ds(0, 5)],
            group_of(d, GROUPS),
            rows=peer[d],
        ).start()
    for k in range(1, NCHAN):
        pl.semaphore_signal(ready_sem, 1, device_id={"chan": other[k]}, device_id_type=MESH)

    start = 0
    for g, group in enumerate(GROUPS):
        if len(group) > (0 in group):
            wait_tiles(arrived, group, g)
        cols = slice(start, start + len(group) * CAP)
        part = accumulate(arrived, group, rows, left, hot, cols)
        start = cols.stop
        if g == 0:
            sums[...] = part
        elif g < len(GROUPS) - 1:
            sums[...] += part

    def field(f):
        at = slice(NCELL * f, NCELL * f + NCELL)
        return part[at] + sums[at]

    count = field(FIELDS)
    inverse = 1.0 / jnp.maximum(count, 1.0)
    means, variances = [], []
    for c in range(CH):
        mean = (field(c) + field(c + 4)) * inverse
        var = jnp.maximum((field(c + 8) + field(c + 12)) * inverse - mean * mean, 0.0)
        means.append(mean)
        variances.append(var)
    own_spread = (variances[0] + variances[1]) + (variances[2] + variances[3])
    spreads[0] = own_spread
    fields = means + [own_spread]
    highs = [high_of(x) for x in fields]
    lows = [x - h for x, h in zip(fields, highs)]
    table[...] = jnp.concatenate(highs + lows, axis=0).astype(BF16)

    def send_partial(d, k):
        remote(
            back.at[d, pl.ds(4, 1)],
            partial.at[pl.ds((k - 1) * NROW + d, 1)],
            first_part,
            rows=peer[d],
            chan=other[k],
        ).start()

    def send_back(d):
        remote(
            back.at[d, pl.ds(0, 5)], returned.at[d, pl.ds(0, 5)], first_back, rows=peer[d]
        ).start()

    nfield = len(fields)
    order = [d for group in GROUPS for d in group]
    turn = 4
    for t in reversed(range(NROW // turn)):
        group = order[turn * t : turn * t + turn]
        lanes = turn * CAP
        looks = jnp.dot(
            table[...], hot[:, lanes * t : lanes * t + lanes], preferred_element_type=F32
        ).reshape(2 * nfield, NCELL, lanes)
        looks = looks[:nfield] + looks[nfield:]
        code = jnp.concatenate(
            [jnp.broadcast_to(arrived[d, 4:5], (8, CAP)) for d in group], axis=1
        )
        cell_hi = jnp.floor(code * (1.0 / 256.0))
        row = iota((8, lanes), 0)
        here = [cell_hi == (row + (8 * i + 1)).astype(F32) for i in range(NCELL // 8)]
        looked = jnp.zeros((8, lanes), F32)
        for f in range(nfield):
            only = jnp.where(here[0], looks[f, 0:8], 0.0)
            for i in range(1, NCELL // 8):
                only = only + jnp.where(here[i], looks[f, 8 * i : 8 * i + 8], 0.0)
            only = only + pltpu.roll(only, 4, 0)
            only = only + pltpu.roll(only, 2, 0)
            only = only + pltpu.roll(only, 1, 0)
            looked = jnp.where(row == f, only, looked)
        tile = jnp.concatenate([arrived[d] for d in group], axis=1)
        tile = jnp.where(row < 4, tile - looked, looked)
        for i, d in enumerate(group):
            back[d] = tile[:, CAP * i : CAP * i + CAP]
        if t == NROW // turn - 1:
            pl.semaphore_wait(ready_sem, NCHAN - 1)
        for k in (2, 1, 3):
            for d in reversed(group):
                send_partial(d, k)
    for d in FAR:
        send_back(d)
    for k in range(1, NCHAN):
        remote(spreads.at[0], spreads.at[k], grid_sem, chan=other[k]).start()

    def to_rows(part, out, grid):
        lo, hi = WIDE * part, min(WIDE * part + WIDE, COLS)
        out[:, lo:hi] = grid[4 * part : 4 * part + 4, 0 : hi - lo].astype(out.dtype)

    returned[0] = back[0]
    for part in range(6):
        to_rows(part, count_out, count)
        for c in range(CH):
            to_rows(part, mean_out.at[c], means[c])
            to_rows(part, var_out.at[c], variances[c])

    wait_tiles(returned, NEAR, first_back)
    packed = returned[...].reshape(NROW * 8, CAP)
    high = high_of(packed)
    pieces = jnp.concatenate([high, packed - high], axis=1).astype(BF16)
    lanes = 512
    for t in range(OBS // lanes):
        cols = slice(t * lanes, t * lanes + lanes)
        twice = jnp.concatenate([right[:, cols], right[:, cols]], axis=0)
        found = jnp.dot(pieces, twice, preferred_element_type=F32)
        names = jnp.broadcast_to(brel[:, cols], (8, lanes))
        total = jnp.zeros((8, lanes), F32)
        for d in range(NROW):
            total = total + jnp.where(names == float(d), found[8 * d : 8 * d + 8], 0.0)
        shifted_ref[:, cols] = total[0:4]
    for d in range(NROW):
        slots_ref[d : d + 1] = returned[d, 4:5]
    waited = spreads.at[pl.ds(1, NCHAN - 1)]
    remote(waited, waited, grid_sem, rows=me).wait()
    spread = (spreads[0] + spreads[1]) + (spreads[2] + spreads[3])
    for part in range(6):
        to_rows(part, spread_out, spread)
    remote(partial, partial, first_part, rows=me).wait()
    rest = (partial[0:NROW] + partial[NROW : 2 * NROW]) + partial[2 * NROW :]
    slots_ref[...] += rest


def last_kernel(
    count_ref,
    mean_ref,
    var_ref,
    spread_ref,
    shifted_ref,
    slots_ref,
    rank_ref,
    brel,
    count_hbm,
    mean_hbm,
    var_hbm,
    spread_hbm,
    dep_hbm,
    dep_ref,
    sem,
):
    pairs = (
        (mean_ref, mean_hbm),
        (var_ref, var_hbm),
        (count_ref, count_hbm),
        (spread_ref, spread_hbm),
        (dep_ref, dep_hbm),
    )
    copies = [
        pltpu.make_async_copy(src, dst, sem.at[i]) for i, (src, dst) in enumerate(pairs)
    ]
    for copy in copies[:4]:
        copy.start()
    table = [slots_ref[8 * i : 8 * i + 8] for i in range(NROW // 8)]
    row = iota((8, CAP), 0)
    for t in range(OBS // CAP):
        cols = slice(t * CAP, t * CAP + CAP)
        at = jnp.broadcast_to(rank_ref[:, cols], (8, CAP)).astype(jnp.int32)
        names = jnp.broadcast_to(brel[:, cols], (8, CAP)).astype(jnp.int32)
        spread = jnp.zeros((8, CAP), F32)
        for i, lines in enumerate(table):
            there = jnp.take_along_axis(lines, at, axis=1, mode="promise_in_bounds")
            spread = spread + jnp.where(names == row + 8 * i, there, 0.0)
        spread = spread + pltpu.roll(spread, 4, 0)
        spread = spread + pltpu.roll(spread, 2, 0)
        spread = spread + pltpu.roll(spread, 1, 0)
        dep_ref[:, cols] = shifted_ref[:, cols] * lax.rsqrt(1.0 + spread[0:4] / CHAN)
    copies[4].start()
    for copy in copies:
        copy.wait()


def body(radiances, band, row_in_band, column):
    vmem = pl.BlockSpec(memory_space=pltpu.VMEM)
    hbm = pl.BlockSpec(memory_space=pltpu.HBM)
    shape = jax.ShapeDtypeStruct
    grid = (NCELL, WIDE)
    outs = (
        shape((4, COLS), jnp.int32),
        shape((CH, 4, COLS), F32),
        shape((CH, 4, COLS), F32),
        shape((4, COLS), F32),
        shape((CH, OBS), F32),
    )
    between = (
        *outs[:4],
        shape((CH, OBS), F32),
        shape((NROW, CAP), F32),
        shape((1, OBS), F32),
        shape((1, OBS), F32),
    )
    nsem = len(GROUPS) + 2 * len(BACK) + 1
    operands = (
        radiances,
        band.reshape(1, OBS),
        row_in_band.reshape(1, OBS),
        column.reshape(1, OBS),
    )
    made = pl.pallas_call(
        comm_kernel,
        out_shape=between,
        in_specs=[hbm] * 4,
        out_specs=(vmem,) * 8,
        scratch_shapes=[
            pltpu.VMEM((CH, OBS), F32),
            pltpu.VMEM((1, OBS), jnp.int32),
            pltpu.VMEM((1, OBS), jnp.int32),
            pltpu.VMEM((1, OBS), jnp.int32),
            pltpu.VMEM((16 * NROW, OBS), BF16),
            pltpu.VMEM((CAP, OBS), BF16),
            pltpu.VMEM((NROW, 8, CAP), F32),
            pltpu.VMEM((NROW, 8, CAP), F32),
            pltpu.VMEM((FIELDS, 22 * CAP), F32),
            pltpu.VMEM((WIDE, NROW * CAP), BF16),
            pltpu.VMEM((FIELDS * NCELL + 32, WIDE), F32),
            pltpu.VMEM((10 * NCELL, WIDE), BF16),
            pltpu.VMEM((NROW, 8, CAP), F32),
            pltpu.VMEM((NROW, 8, CAP), F32),
            pltpu.VMEM(((NCHAN - 1) * NROW, CAP), F32),
            pltpu.VMEM((NCHAN, *grid), F32),
            pltpu.SemaphoreType.DMA((nsem,)),
            pltpu.SemaphoreType.DMA((nsem,)),
            pltpu.SemaphoreType.REGULAR,
            pltpu.SemaphoreType.DMA((4,)),
        ],
        compiler_params=pltpu.CompilerParams(
            collective_id=0, has_side_effects=True, vmem_limit_bytes=24 << 20
        ),
    )(*(pltpu.with_memory_space_constraint(x, pltpu.HBM) for x in operands))
    return pl.pallas_call(
        last_kernel,
        out_shape=outs,
        in_specs=[vmem] * 8,
        out_specs=(hbm,) * 5,
        scratch_shapes=[pltpu.VMEM((CH, OBS), F32), pltpu.SemaphoreType.DMA((5,))],
        compiler_params=pltpu.CompilerParams(vmem_limit_bytes=16 << 20),
    )(*made)


def solution(mesh):
    in_specs = (P("chan", "rows"), P("rows", None), P("rows"), P("rows"))
    out_specs = (
        P("rows", None),
        P("chan", "rows", None),
        P("chan", "rows", None),
        P("rows", None),
        P("chan", "rows"),
    )
    return jax.shard_map(body, mesh=mesh, in_specs=in_specs, out_specs=out_specs, check_vma=False)
```

```python
import functools

import jax
import jax.numpy as jnp
from jax import lax
from jax.experimental import pallas as pl
from jax.experimental.pallas import tpu as pltpu
from jax.sharding import PartitionSpec as P

CHAN = 16
COLS = 1440
NROW = 32
NCHAN = 4
CH = 4
OBS = 2048
CAP = 128
WIDE = 256
NCELL = 24
MESH = pl.DeviceIdType.MESH
F32 = jnp.float32
BF16 = jnp.bfloat16


def hops(offset):
    ring = (0, 1, 2, 1)
    return ring[offset >> 3] + ring[(offset >> 1) & 3]


NEAR = tuple(sorted(range(NROW), key=hops))
FAR = tuple(d for d in reversed(NEAR) if d)
GROUPS = (NEAR[0:8], NEAR[8:20], NEAR[20:28], NEAR[28:32])
BACK = (NEAR,)
FIELDS = 16


def iota(shape, dim):
    return lax.broadcasted_iota(jnp.int32, shape, dim)


def rows16(row):
    return jnp.broadcast_to(row, (16, row.shape[1])).astype(BF16)


def count16(lanes):
    return iota((16, lanes), 0).astype(F32).astype(BF16)


def hot_into(ref, top, cols, names, blocks, lanes, first=0):
    one, zero = jnp.ones((16, lanes), BF16), jnp.zeros((16, lanes), BF16)
    steps = count16(lanes)
    for k in range(blocks):
        ref[top + 16 * k : top + 16 * k + 16, cols] = jnp.where(
            names == steps + jnp.asarray(16 * k + first, BF16), one, zero
        )


def high_of(x):
    return x.astype(BF16).astype(F32)


def spread_into_slots(radiances, bands, rib, column, left, right, rank_ref, tiles):
    lanes = OBS
    names = rows16(bands)
    hot_into(right, 0, slice(0, lanes), names, 2, lanes)
    blocks = [right[0:32, WIDE * j : WIDE * j + WIDE] for j in range(OBS // WIDE)]
    before, seen = [], jnp.zeros((32, WIDE), BF16)
    for block in blocks:
        before.append(seen)
        seen = seen + block
    stacked = jnp.concatenate(
        [jnp.concatenate(before, axis=0), jnp.concatenate(blocks, axis=0)], axis=1
    )
    ones = jnp.ones((WIDE, WIDE), BF16)
    upper = jnp.where(iota((WIDE, WIDE), 0) <= iota((WIDE, WIDE), 1), 1.0, 0.0).astype(BF16)
    prefix = jnp.dot(
        stacked, jnp.concatenate([ones, upper], axis=0), preferred_element_type=F32
    )
    ranks = []
    for j, block in enumerate(blocks):
        own = block.astype(F32) * prefix[32 * j : 32 * j + 32]
        ranks.append(jnp.sum(own, axis=0, keepdims=True) - 1.0)
    rank = jnp.concatenate(ranks, axis=1)
    rank_ref[...] = rank
    hot_into(right, 0, slice(0, lanes), rows16(rank), CAP // 16, lanes)

    row = iota((8, lanes), 0)
    both = jnp.concatenate([radiances, radiances], axis=0)
    high = high_of(both)
    middle = high_of(both - high)
    low = both - high - middle
    cell_hi = jnp.broadcast_to(((column >> 8) * 4 + rib + 1).astype(F32), (8, lanes))
    cell_lo = jnp.broadcast_to((column & 255).astype(F32), (8, lanes))
    names_of = jnp.where(row == 4, cell_hi, jnp.where(row == 5, cell_lo, 0.0))
    payload = jnp.concatenate(
        [jnp.where(row < 4, high, middle), jnp.where(row < 4, low, names_of)], axis=0
    ).astype(BF16)
    zero = jnp.zeros((16, lanes), BF16)
    for b in range(NROW):
        left[16 * b : 16 * b + 16, :] = jnp.where(names == jnp.asarray(b, BF16), payload, zero)
    placed = lax.dot_general(
        left[...], right[...], (((1,), (1,)), ((), ())), preferred_element_type=F32
    ).reshape(NROW, 16, CAP)
    upper_half, lower_half = placed[:, :8], placed[:, 8:]
    tile_row = iota((NROW, 8, CAP), 1)
    total = upper_half + pltpu.roll(upper_half, 4, 1) + lower_half
    tiles[...] = jnp.where(
        tile_row < 4, total, lower_half * 256.0 + pltpu.roll(lower_half, 7, 1)
    )


def feature_rows(ref, f1, f2, lanes):
    first = jnp.broadcast_to(ref[f1 : f1 + 1, 0:lanes], (8, lanes))
    second = jnp.broadcast_to(ref[f2 : f2 + 1, 0:lanes], (8, lanes))
    return [
        jnp.concatenate(pair, axis=0).astype(BF16)
        for pair in ((first, first), (first, second), (second, second))
    ]


def accumulate(arrived, group, rows, left, hot, cols):
    lanes = len(group) * CAP
    row = iota((8, lanes), 0)
    tile = jnp.concatenate([arrived[d] for d in group], axis=1)
    code = jnp.concatenate(
        [jnp.broadcast_to(arrived[d, 4:5], (8, CAP)) for d in group], axis=1
    )
    value = jnp.where(row < 4, tile, pltpu.roll(tile, 4, 0))
    square = value * value
    value_hi, square_hi = high_of(value), high_of(square)
    rows[0:8, 0:lanes] = jnp.where(row < 4, value_hi, value - value_hi)
    rows[8:16, 0:lanes] = jnp.where(row < 4, square_hi, square - square_hi)
    cell_hi = jnp.floor(code * (1.0 / 256.0))
    cell_lo = code - 256.0 * cell_hi
    hi16 = jnp.concatenate([cell_hi, cell_hi], axis=0).astype(BF16)
    lo16 = jnp.concatenate([cell_lo, cell_lo], axis=0).astype(BF16)
    step = iota((16, lanes), 0)
    names = (step + 1, jnp.where(step < 8, step + 17, step - 7), step + 9)
    masks = [hi16 == n.astype(F32).astype(BF16) for n in names]
    zero = jnp.zeros((16, lanes), BF16)
    for pair in range(FIELDS // 2):
        for i, source in enumerate(feature_rows(rows, 2 * pair, 2 * pair + 1, lanes)):
            at = 48 * pair + 16 * i
            left[at : at + 16, 0:lanes] = jnp.where(masks[i], source, zero)
    hot_into(left, FIELDS * NCELL, slice(0, lanes), hi16, 2, lanes, first=1)
    hot_into(hot, 0, cols, lo16, WIDE // 16, lanes)
    return lax.dot_general(
        left[0 : FIELDS * NCELL + 32, 0:lanes],
        hot[:, cols],
        (((1,), (1,)), ((), ())),
        preferred_element_type=F32,
    )


def comm_kernel(
    rad_hbm,
    band_hbm,
    rib_hbm,
    col_hbm,
    count_out,
    mean_out,
    var_out,
    spread_out,
    shifted_ref,
    slots_ref,
    rank_ref,
    brel,
    rad_ref,
    band_ref,
    rib_ref,
    col_ref,
    left,
    right,
    tiles,
    arrived,
    rows,
    hot,
    sums,
    table,
    back,
    returned,
    partial,
    spreads,
    send_sem,
    recv_sem,
    ready_sem,
    load_sem,
):
    loads = [
        pltpu.make_async_copy(src, dst, load_sem.at[i])
        for i, (src, dst) in enumerate(
            ((band_hbm, band_ref), (rad_hbm, rad_ref), (rib_hbm, rib_ref), (col_hbm, col_ref))
        )
    ]
    for load in loads:
        load.start()
    me, mine = lax.axis_index("rows"), lax.axis_index("chan")
    peer = {d: lax.bitwise_xor(me, d) for d in range(NROW)}
    other = {k: lax.bitwise_xor(mine, k) for k in range(NCHAN)}
    barrier = pltpu.get_barrier_semaphore()
    for d in FAR:
        pl.semaphore_signal(barrier, 1, device_id={"rows": peer[d]}, device_id_type=MESH)
    for k in range(1, NCHAN):
        pl.semaphore_signal(barrier, 1, device_id={"chan": other[k]}, device_id_type=MESH)

    for load in loads:
        load.wait()
    bands = lax.bitwise_xor(band_ref[...], me).astype(F32)
    brel[...] = bands
    spread_into_slots(
        rad_ref[...], bands, rib_ref[...], col_ref[...], left, right, rank_ref, tiles
    )
    arrived[0] = tiles[0]
    pl.semaphore_wait(barrier, NROW - 1 + NCHAN - 1)

    def remote(src, dst, which, **to):
        return pltpu.make_async_remote_copy(
            src_ref=src,
            dst_ref=dst,
            send_sem=send_sem.at[which],
            recv_sem=recv_sem.at[which],
            device_id=to,
            device_id_type=MESH,
        )

    def group_of(d, groups):
        return [d in group for group in groups].index(True)

    def wait_tiles(buffer, group, which):
        part = buffer.at[pl.ds(0, len(group) - (0 in group)), pl.ds(0, 5)]
        remote(part, part, which, rows=me).wait()

    first_back = len(GROUPS)
    first_part = first_back + len(BACK)
    grid_sem = first_part + len(BACK)

    for d in FAR:
        remote(
            tiles.at[d, pl.ds(0, 5)],
            arrived.at[d, pl.ds(0, 5)],
            group_of(d, GROUPS),
            rows=peer[d],
        ).start()
    for k in range(1, NCHAN):
        pl.semaphore_signal(ready_sem, 1, device_id={"chan": other[k]}, device_id_type=MESH)

    start = 0
    for g, group in enumerate(GROUPS):
        if len(group) > (0 in group):
            wait_tiles(arrived, group, g)
        cols = slice(start, start + len(group) * CAP)
        part = accumulate(arrived, group, rows, left, hot, cols)
        start = cols.stop
        if g == 0:
            sums[...] = part
        elif g < len(GROUPS) - 1:
            sums[...] += part

    def field(f):
        at = slice(NCELL * f, NCELL * f + NCELL)
        return part[at] + sums[at]

    count = field(FIELDS)
    inverse = 1.0 / jnp.maximum(count, 1.0)
    means, variances = [], []
    for c in range(CH):
        mean = (field(c) + field(c + 4)) * inverse
        var = jnp.maximum((field(c + 8) + field(c + 12)) * inverse - mean * mean, 0.0)
        means.append(mean)
        variances.append(var)
    own_spread = (variances[0] + variances[1]) + (variances[2] + variances[3])
    spreads[0] = own_spread
    fields = means + [own_spread]
    highs = [high_of(x) for x in fields]
    lows = [x - h for x, h in zip(fields, highs)]
    table[...] = jnp.concatenate(highs + lows, axis=0).astype(BF16)

    def send_partial(d, k):
        remote(
            back.at[d, pl.ds(4, 1)],
            partial.at[pl.ds((k - 1) * NROW + d, 1)],
            first_part,
            rows=peer[d],
            chan=other[k],
        ).start()

    def send_back(d):
        remote(
            back.at[d, pl.ds(0, 5)], returned.at[d, pl.ds(0, 5)], first_back, rows=peer[d]
        ).start()

    nfield = len(fields)
    order = [d for group in GROUPS for d in group]
    turn = 4
    for t in reversed(range(NROW // turn)):
        group = order[turn * t : turn * t + turn]
        lanes = turn * CAP
        looks = jnp.dot(
            table[...], hot[:, lanes * t : lanes * t + lanes], preferred_element_type=F32
        ).reshape(2 * nfield, NCELL, lanes)
        looks = looks[:nfield] + looks[nfield:]
        code = jnp.concatenate(
            [jnp.broadcast_to(arrived[d, 4:5], (8, CAP)) for d in group], axis=1
        )
        cell_hi = jnp.floor(code * (1.0 / 256.0))
        row = iota((8, lanes), 0)
        here = [cell_hi == (row + (8 * i + 1)).astype(F32) for i in range(NCELL // 8)]
        looked = jnp.zeros((8, lanes), F32)
        for f in range(nfield):
            only = jnp.where(here[0], looks[f, 0:8], 0.0)
            for i in range(1, NCELL // 8):
                only = only + jnp.where(here[i], looks[f, 8 * i : 8 * i + 8], 0.0)
            only = only + pltpu.roll(only, 4, 0)
            only = only + pltpu.roll(only, 2, 0)
            only = only + pltpu.roll(only, 1, 0)
            looked = jnp.where(row == f, only, looked)
        tile = jnp.concatenate([arrived[d] for d in group], axis=1)
        tile = jnp.where(row < 4, tile - looked, looked)
        for i, d in enumerate(group):
            back[d] = tile[:, CAP * i : CAP * i + CAP]
        if t == NROW // turn - 1:
            pl.semaphore_wait(ready_sem, NCHAN - 1)
        for k in (2, 1, 3):
            for d in reversed(group):
                send_partial(d, k)
    for d in FAR:
        send_back(d)
    for k in range(1, NCHAN):
        remote(spreads.at[0], spreads.at[k], grid_sem, chan=other[k]).start()

    def to_rows(part, out, grid):
        lo, hi = WIDE * part, min(WIDE * part + WIDE, COLS)
        out[:, lo:hi] = grid[4 * part : 4 * part + 4, 0 : hi - lo].astype(out.dtype)

    returned[0] = back[0]
    for part in range(6):
        to_rows(part, count_out, count)
        for c in range(CH):
            to_rows(part, mean_out.at[c], means[c])
            to_rows(part, var_out.at[c], variances[c])

    wait_tiles(returned, NEAR, first_back)
    packed = returned[...].reshape(NROW * 8, CAP)
    high = high_of(packed)
    pieces = jnp.concatenate([high, packed - high], axis=1).astype(BF16)
    lanes = 512
    for t in range(OBS // lanes):
        cols = slice(t * lanes, t * lanes + lanes)
        twice = jnp.concatenate([right[:, cols], right[:, cols]], axis=0)
        found = jnp.dot(pieces, twice, preferred_element_type=F32)
        names = jnp.broadcast_to(brel[:, cols], (8, lanes))
        total = jnp.zeros((8, lanes), F32)
        for d in range(NROW):
            total = total + jnp.where(names == float(d), found[8 * d : 8 * d + 8], 0.0)
        shifted_ref[:, cols] = total[0:4]
    for d in range(NROW):
        slots_ref[d : d + 1] = returned[d, 4:5]
    waited = spreads.at[pl.ds(1, NCHAN - 1)]
    remote(waited, waited, grid_sem, rows=me).wait()
    spread = (spreads[0] + spreads[1]) + (spreads[2] + spreads[3])
    for part in range(6):
        to_rows(part, spread_out, spread)
    remote(partial, partial, first_part, rows=me).wait()
    rest = (partial[0:NROW] + partial[NROW : 2 * NROW]) + partial[2 * NROW :]
    slots_ref[...] += rest


def last_kernel(
    count_ref,
    mean_ref,
    var_ref,
    spread_ref,
    shifted_ref,
    slots_ref,
    rank_ref,
    brel,
    count_hbm,
    mean_hbm,
    var_hbm,
    spread_hbm,
    dep_hbm,
    dep_ref,
    sem,
):
    pairs = (
        (mean_ref, mean_hbm),
        (var_ref, var_hbm),
        (count_ref, count_hbm),
        (spread_ref, spread_hbm),
        (dep_ref, dep_hbm),
    )
    copies = [
        pltpu.make_async_copy(src, dst, sem.at[i]) for i, (src, dst) in enumerate(pairs)
    ]
    for copy in copies[:4]:
        copy.start()
    table = [slots_ref[8 * i : 8 * i + 8] for i in range(NROW // 8)]
    row = iota((8, CAP), 0)
    for t in range(OBS // CAP):
        cols = slice(t * CAP, t * CAP + CAP)
        at = jnp.broadcast_to(rank_ref[:, cols], (8, CAP)).astype(jnp.int32)
        names = jnp.broadcast_to(brel[:, cols], (8, CAP)).astype(jnp.int32)
        spread = jnp.zeros((8, CAP), F32)
        for i, lines in enumerate(table):
            there = jnp.take_along_axis(lines, at, axis=1, mode="promise_in_bounds")
            spread = spread + jnp.where(names == row + 8 * i, there, 0.0)
        spread = spread + pltpu.roll(spread, 4, 0)
        spread = spread + pltpu.roll(spread, 2, 0)
        spread = spread + pltpu.roll(spread, 1, 0)
        dep_ref[:, cols] = shifted_ref[:, cols] * lax.rsqrt(1.0 + spread[0:4] / CHAN)
    copies[4].start()
    for copy in copies:
        copy.wait()


def body(radiances, band, row_in_band, column):
    vmem = pl.BlockSpec(memory_space=pltpu.VMEM)
    hbm = pl.BlockSpec(memory_space=pltpu.HBM)
    shape = jax.ShapeDtypeStruct
    grid = (NCELL, WIDE)
    outs = (
        shape((4, COLS), jnp.int32),
        shape((CH, 4, COLS), F32),
        shape((CH, 4, COLS), F32),
        shape((4, COLS), F32),
        shape((CH, OBS), F32),
    )
    between = (
        *outs[:4],
        shape((CH, OBS), F32),
        shape((NROW, CAP), F32),
        shape((1, OBS), F32),
        shape((1, OBS), F32),
    )
    nsem = len(GROUPS) + 2 * len(BACK) + 1
    operands = (
        radiances,
        band.reshape(1, OBS),
        row_in_band.reshape(1, OBS),
        column.reshape(1, OBS),
    )
    made = pl.pallas_call(
        comm_kernel,
        out_shape=between,
        in_specs=[hbm] * 4,
        out_specs=(vmem,) * 8,
        scratch_shapes=[
            pltpu.VMEM((CH, OBS), F32),
            pltpu.VMEM((1, OBS), jnp.int32),
            pltpu.VMEM((1, OBS), jnp.int32),
            pltpu.VMEM((1, OBS), jnp.int32),
            pltpu.VMEM((16 * NROW, OBS), BF16),
            pltpu.VMEM((CAP, OBS), BF16),
            pltpu.VMEM((NROW, 8, CAP), F32),
            pltpu.VMEM((NROW, 8, CAP), F32),
            pltpu.VMEM((FIELDS, 22 * CAP), F32),
            pltpu.VMEM((WIDE, NROW * CAP), BF16),
            pltpu.VMEM((FIELDS * NCELL + 32, WIDE), F32),
            pltpu.VMEM((10 * NCELL, WIDE), BF16),
            pltpu.VMEM((NROW, 8, CAP), F32),
            pltpu.VMEM((NROW, 8, CAP), F32),
            pltpu.VMEM(((NCHAN - 1) * NROW, CAP), F32),
            pltpu.VMEM((NCHAN, *grid), F32),
            pltpu.SemaphoreType.DMA((nsem,)),
            pltpu.SemaphoreType.DMA((nsem,)),
            pltpu.SemaphoreType.REGULAR,
            pltpu.SemaphoreType.DMA((4,)),
        ],
        compiler_params=pltpu.CompilerParams(
            collective_id=0, has_side_effects=True, vmem_limit_bytes=24 << 20
        ),
    )(*(pltpu.with_memory_space_constraint(x, pltpu.HBM) for x in operands))
    return pl.pallas_call(
        last_kernel,
        out_shape=outs,
        in_specs=[vmem] * 8,
        out_specs=(hbm,) * 5,
        scratch_shapes=[pltpu.VMEM((CH, OBS), F32), pltpu.SemaphoreType.DMA((5,))],
        compiler_params=pltpu.CompilerParams(vmem_limit_bytes=16 << 20),
    )(*made)


def solution(mesh):
    in_specs = (P("chan", "rows"), P("rows", None), P("rows"), P("rows"))
    out_specs = (
        P("rows", None),
        P("chan", "rows", None),
        P("chan", "rows", None),
        P("rows", None),
        P("chan", "rows"),
    )
    return jax.shard_map(body, mesh=mesh, in_specs=in_specs, out_specs=out_specs, check_vma=False)
```

```python
import functools

import jax
import jax.numpy as jnp
from jax import lax
from jax.experimental import pallas as pl
from jax.experimental.pallas import tpu as pltpu
from jax.sharding import PartitionSpec as P

CHAN = 16
COLS = 1440
NROW = 32
NCHAN = 4
CH = 4
OBS = 2048
CAP = 128
WIDE = 256
NCELL = 24
MESH = pl.DeviceIdType.MESH
F32 = jnp.float32
BF16 = jnp.bfloat16


def hops(offset):
    ring = (0, 1, 2, 1)
    return ring[offset >> 3] + ring[(offset >> 1) & 3]


NEAR = tuple(sorted(range(NROW), key=hops))
FAR = tuple(d for d in reversed(NEAR) if d)
GROUPS = (NEAR[0:8], NEAR[8:20], NEAR[20:28], NEAR[28:32])
BACK = (NEAR,)
FIELDS = 16


def iota(shape, dim):
    return lax.broadcasted_iota(jnp.int32, shape, dim)


def rows16(row):
    return jnp.broadcast_to(row, (16, row.shape[1])).astype(BF16)


def count16(lanes):
    return iota((16, lanes), 0).astype(F32).astype(BF16)


def hot_into(ref, top, cols, names, blocks, lanes, first=0):
    one, zero = jnp.ones((16, lanes), BF16), jnp.zeros((16, lanes), BF16)
    steps = count16(lanes)
    for k in range(blocks):
        ref[top + 16 * k : top + 16 * k + 16, cols] = jnp.where(
            names == steps + jnp.asarray(16 * k + first, BF16), one, zero
        )


def high_of(x):
    return x.astype(BF16).astype(F32)


def spread_into_slots(radiances, bands, rib, column, left, right, rank_ref, tiles):
    lanes = OBS
    names = rows16(bands)
    hot_into(right, 0, slice(0, lanes), names, 2, lanes)
    blocks = [right[0:32, WIDE * j : WIDE * j + WIDE] for j in range(OBS // WIDE)]
    before, seen = [], jnp.zeros((32, WIDE), BF16)
    for block in blocks:
        before.append(seen)
        seen = seen + block
    stacked = jnp.concatenate(
        [jnp.concatenate(before, axis=0), jnp.concatenate(blocks, axis=0)], axis=1
    )
    ones = jnp.ones((WIDE, WIDE), BF16)
    upper = jnp.where(iota((WIDE, WIDE), 0) <= iota((WIDE, WIDE), 1), 1.0, 0.0).astype(BF16)
    prefix = jnp.dot(
        stacked, jnp.concatenate([ones, upper], axis=0), preferred_element_type=F32
    )
    ranks = []
    for j, block in enumerate(blocks):
        own = block.astype(F32) * prefix[32 * j : 32 * j + 32]
        ranks.append(jnp.sum(own, axis=0, keepdims=True) - 1.0)
    rank = jnp.concatenate(ranks, axis=1)
    rank_ref[...] = rank
    hot_into(right, 0, slice(0, lanes), rows16(rank), CAP // 16, lanes)

    row = iota((8, lanes), 0)
    both = jnp.concatenate([radiances, radiances], axis=0)
    high = high_of(both)
    middle = high_of(both - high)
    low = both - high - middle
    cell_hi = jnp.broadcast_to(((column >> 8) * 4 + rib + 1).astype(F32), (8, lanes))
    cell_lo = jnp.broadcast_to((column & 255).astype(F32), (8, lanes))
    names_of = jnp.where(row == 4, cell_hi, jnp.where(row == 5, cell_lo, 0.0))
    payload = jnp.concatenate(
        [jnp.where(row < 4, high, middle), jnp.where(row < 4, low, names_of)], axis=0
    ).astype(BF16)
    zero = jnp.zeros((16, lanes), BF16)
    for b in range(NROW):
        left[16 * b : 16 * b + 16, :] = jnp.where(names == jnp.asarray(b, BF16), payload, zero)
    placed = lax.dot_general(
        left[...], right[...], (((1,), (1,)), ((), ())), preferred_element_type=F32
    ).reshape(NROW, 16, CAP)
    upper_half, lower_half = placed[:, :8], placed[:, 8:]
    tile_row = iota((NROW, 8, CAP), 1)
    total = upper_half + pltpu.roll(upper_half, 4, 1) + lower_half
    tiles[...] = jnp.where(
        tile_row < 4, total, lower_half * 256.0 + pltpu.roll(lower_half, 7, 1)
    )


def feature_rows(ref, f1, f2, lanes):
    first = jnp.broadcast_to(ref[f1 : f1 + 1, 0:lanes], (8, lanes))
    second = jnp.broadcast_to(ref[f2 : f2 + 1, 0:lanes], (8, lanes))
    return [
        jnp.concatenate(pair, axis=0).astype(BF16)
        for pair in ((first, first), (first, second), (second, second))
    ]


def accumulate(arrived, group, rows, left, hot, cols):
    lanes = len(group) * CAP
    row = iota((8, lanes), 0)
    tile = jnp.concatenate([arrived[d] for d in group], axis=1)
    code = jnp.concatenate(
        [jnp.broadcast_to(arrived[d, 4:5], (8, CAP)) for d in group], axis=1
    )
    value = jnp.where(row < 4, tile, pltpu.roll(tile, 4, 0))
    square = value * value
    value_hi, square_hi = high_of(value), high_of(square)
    rows[0:8, 0:lanes] = jnp.where(row < 4, value_hi, value - value_hi)
    rows[8:16, 0:lanes] = jnp.where(row < 4, square_hi, square - square_hi)
    cell_hi = jnp.floor(code * (1.0 / 256.0))
    cell_lo = code - 256.0 * cell_hi
    hi16 = jnp.concatenate([cell_hi, cell_hi], axis=0).astype(BF16)
    lo16 = jnp.concatenate([cell_lo, cell_lo], axis=0).astype(BF16)
    step = iota((16, lanes), 0)
    names = (step + 1, jnp.where(step < 8, step + 17, step - 7), step + 9)
    masks = [hi16 == n.astype(F32).astype(BF16) for n in names]
    zero = jnp.zeros((16, lanes), BF16)
    for pair in range(FIELDS // 2):
        for i, source in enumerate(feature_rows(rows, 2 * pair, 2 * pair + 1, lanes)):
            at = 48 * pair + 16 * i
            left[at : at + 16, 0:lanes] = jnp.where(masks[i], source, zero)
    hot_into(left, FIELDS * NCELL, slice(0, lanes), hi16, 2, lanes, first=1)
    hot_into(hot, 0, cols, lo16, WIDE // 16, lanes)
    return lax.dot_general(
        left[0 : FIELDS * NCELL + 32, 0:lanes],
        hot[:, cols],
        (((1,), (1,)), ((), ())),
        preferred_element_type=F32,
    )


def comm_kernel(
    rad_hbm,
    band_hbm,
    rib_hbm,
    col_hbm,
    count_out,
    mean_out,
    var_out,
    spread_out,
    shifted_ref,
    slots_ref,
    rank_ref,
    brel,
    rad_ref,
    band_ref,
    rib_ref,
    col_ref,
    left,
    right,
    tiles,
    arrived,
    rows,
    hot,
    sums,
    table,
    own,
    back,
    returned,
    partial,
    spreads,
    send_sem,
    recv_sem,
    ready_sem,
    load_sem,
):
    loads = [
        pltpu.make_async_copy(src, dst, load_sem.at[i])
        for i, (src, dst) in enumerate(
            ((band_hbm, band_ref), (rad_hbm, rad_ref), (rib_hbm, rib_ref), (col_hbm, col_ref))
        )
    ]
    for load in loads:
        load.start()
    me, mine = lax.axis_index("rows"), lax.axis_index("chan")
    peer = {d: lax.bitwise_xor(me, d) for d in range(NROW)}
    other = {k: lax.bitwise_xor(mine, k) for k in range(NCHAN)}
    barrier = pltpu.get_barrier_semaphore()
    for d in FAR:
        pl.semaphore_signal(barrier, 1, device_id={"rows": peer[d]}, device_id_type=MESH)
    for k in range(1, NCHAN):
        pl.semaphore_signal(barrier, 1, device_id={"chan": other[k]}, device_id_type=MESH)

    for load in loads:
        load.wait()
    bands = lax.bitwise_xor(band_ref[...], me).astype(F32)
    brel[...] = bands
    spread_into_slots(
        rad_ref[...], bands, rib_ref[...], col_ref[...], left, right, rank_ref, tiles
    )
    arrived[0] = tiles[0]
    pl.semaphore_wait(barrier, NROW - 1 + NCHAN - 1)

    def remote(src, dst, which, **to):
        return pltpu.make_async_remote_copy(
            src_ref=src,
            dst_ref=dst,
            send_sem=send_sem.at[which],
            recv_sem=recv_sem.at[which],
            device_id=to,
            device_id_type=MESH,
        )

    def group_of(d, groups):
        return [d in group for group in groups].index(True)

    def wait_tiles(buffer, group, which):
        part = buffer.at[pl.ds(0, len(group) - (0 in group)), pl.ds(0, 5)]
        remote(part, part, which, rows=me).wait()

    first_back = len(GROUPS)
    first_part = first_back + len(BACK)
    grid_sem = first_part + len(BACK)

    for d in FAR:
        remote(
            tiles.at[d, pl.ds(0, 5)],
            arrived.at[d, pl.ds(0, 5)],
            group_of(d, GROUPS),
            rows=peer[d],
        ).start()
    for k in range(1, NCHAN):
        pl.semaphore_signal(ready_sem, 1, device_id={"chan": other[k]}, device_id_type=MESH)

    start = 0
    for g, group in enumerate(GROUPS):
        if len(group) > (0 in group):
            wait_tiles(arrived, group, g)
        cols = slice(start, start + len(group) * CAP)
        part = accumulate(arrived, group, rows, left, hot, cols)
        start = cols.stop
        if g == 0:
            sums[...] = part
        elif g < len(GROUPS) - 1:
            sums[...] += part

    def field(f):
        at = slice(NCELL * f, NCELL * f + NCELL)
        return part[at] + sums[at]

    count = field(FIELDS)
    inverse = 1.0 / jnp.maximum(count, 1.0)
    means, variances = [], []
    for c in range(CH):
        mean = (field(c) + field(c + 4)) * inverse
        var = jnp.maximum((field(c + 8) + field(c + 12)) * inverse - mean * mean, 0.0)
        means.append(mean)
        variances.append(var)
    own_spread = (variances[0] + variances[1]) + (variances[2] + variances[3])
    spreads[0] = own_spread
    fields = means + [own_spread]
    highs = [high_of(x) for x in fields]
    lows = [x - h for x, h in zip(fields, highs)]
    table[...] = jnp.concatenate(
        [highs[CH], lows[CH], *highs[:CH], *lows[:CH]], axis=0
    ).astype(BF16)

    def send_partial(d, k):
        remote(
            own.at[pl.ds(d, 1)],
            partial.at[pl.ds((k - 1) * NROW + d, 1)],
            first_part,
            rows=peer[d],
            chan=other[k],
        ).start()

    def send_back(d):
        remote(
            back.at[d, pl.ds(0, 5)], returned.at[d, pl.ds(0, 5)], first_back, rows=peer[d]
        ).start()

    order = [d for group in GROUPS for d in group]

    def look(lines, group, t, nfield):
        lanes = len(group) * CAP
        looks = jnp.dot(
            table[lines, :], hot[:, lanes * t : lanes * t + lanes], preferred_element_type=F32
        ).reshape(2 * nfield, NCELL, lanes)
        looks = looks[:nfield] + looks[nfield:]
        code = jnp.concatenate(
            [jnp.broadcast_to(arrived[d, 4:5], (8, CAP)) for d in group], axis=1
        )
        cell_hi = jnp.floor(code * (1.0 / 256.0))
        row = iota((8, lanes), 0)
        here = [cell_hi == (row + (8 * i + 1)).astype(F32) for i in range(NCELL // 8)]
        result = []
        for f in range(nfield):
            only = jnp.where(here[0], looks[f, 0:8], 0.0)
            for i in range(1, NCELL // 8):
                only = only + jnp.where(here[i], looks[f, 8 * i : 8 * i + 8], 0.0)
            only = only + pltpu.roll(only, 4, 0)
            only = only + pltpu.roll(only, 2, 0)
            result.append(only + pltpu.roll(only, 1, 0))
        return result

    turn = 8
    for t in reversed(range(NROW // turn)):
        group = order[turn * t : turn * t + turn]
        (looked,) = look(slice(0, 2 * NCELL), group, t, 1)
        for i, d in enumerate(group):
            own[d : d + 1] = looked[0:1, CAP * i : CAP * i + CAP]
        if t == NROW // turn - 1:
            pl.semaphore_wait(ready_sem, NCHAN - 1)
        for k in (2, 1, 3):
            for d in reversed(group):
                send_partial(d, k)

    turn = 8
    for t in reversed(range(NROW // turn)):
        group = order[turn * t : turn * t + turn]
        row = iota((8, turn * CAP), 0)
        looked = jnp.concatenate(
            [jnp.broadcast_to(own[d : d + 1], (8, CAP)) for d in group], axis=1
        )
        for f, mean in enumerate(look(slice(2 * NCELL, None), group, t, CH)):
            looked = jnp.where(row == f, mean, looked)
        tile = jnp.concatenate([arrived[d] for d in group], axis=1)
        tile = jnp.where(row < 4, tile - looked, looked)
        for i, d in enumerate(group):
            back[d] = tile[:, CAP * i : CAP * i + CAP]
        for d in reversed(group):
            if d:
                send_back(d)
    for k in range(1, NCHAN):
        remote(spreads.at[0], spreads.at[k], grid_sem, chan=other[k]).start()

    def to_rows(part, out, grid):
        lo, hi = WIDE * part, min(WIDE * part + WIDE, COLS)
        out[:, lo:hi] = grid[4 * part : 4 * part + 4, 0 : hi - lo].astype(out.dtype)

    returned[0] = back[0]
    for part in range(6):
        to_rows(part, count_out, count)
        for c in range(CH):
            to_rows(part, mean_out.at[c], means[c])
            to_rows(part, var_out.at[c], variances[c])

    wait_tiles(returned, NEAR, first_back)
    packed = returned[...].reshape(NROW * 8, CAP)
    high = high_of(packed)
    pieces = jnp.concatenate([high, packed - high], axis=1).astype(BF16)
    lanes = 512
    for t in range(OBS // lanes):
        cols = slice(t * lanes, t * lanes + lanes)
        twice = jnp.concatenate([right[:, cols], right[:, cols]], axis=0)
        found = jnp.dot(pieces, twice, preferred_element_type=F32)
        names = jnp.broadcast_to(brel[:, cols], (8, lanes))
        total = jnp.zeros((8, lanes), F32)
        for d in range(NROW):
            total = total + jnp.where(names == float(d), found[8 * d : 8 * d + 8], 0.0)
        shifted_ref[:, cols] = total[0:4]
    for d in range(NROW):
        slots_ref[d : d + 1] = returned[d, 4:5]
    waited = spreads.at[pl.ds(1, NCHAN - 1)]
    remote(waited, waited, grid_sem, rows=me).wait()
    spread = (spreads[0] + spreads[1]) + (spreads[2] + spreads[3])
    for part in range(6):
        to_rows(part, spread_out, spread)
    remote(partial, partial, first_part, rows=me).wait()
    rest = (partial[0:NROW] + partial[NROW : 2 * NROW]) + partial[2 * NROW :]
    slots_ref[...] += rest


def last_kernel(
    count_ref,
    mean_ref,
    var_ref,
    spread_ref,
    shifted_ref,
    slots_ref,
    rank_ref,
    brel,
    count_hbm,
    mean_hbm,
    var_hbm,
    spread_hbm,
    dep_hbm,
    dep_ref,
    sem,
):
    pairs = (
        (mean_ref, mean_hbm),
        (var_ref, var_hbm),
        (count_ref, count_hbm),
        (spread_ref, spread_hbm),
        (dep_ref, dep_hbm),
    )
    copies = [
        pltpu.make_async_copy(src, dst, sem.at[i]) for i, (src, dst) in enumerate(pairs)
    ]
    for copy in copies[:4]:
        copy.start()
    table = [slots_ref[8 * i : 8 * i + 8] for i in range(NROW // 8)]
    row = iota((8, CAP), 0)
    for t in range(OBS // CAP):
        cols = slice(t * CAP, t * CAP + CAP)
        at = jnp.broadcast_to(rank_ref[:, cols], (8, CAP)).astype(jnp.int32)
        names = jnp.broadcast_to(brel[:, cols], (8, CAP)).astype(jnp.int32)
        spread = jnp.zeros((8, CAP), F32)
        for i, lines in enumerate(table):
            there = jnp.take_along_axis(lines, at, axis=1, mode="promise_in_bounds")
            spread = spread + jnp.where(names == row + 8 * i, there, 0.0)
        spread = spread + pltpu.roll(spread, 4, 0)
        spread = spread + pltpu.roll(spread, 2, 0)
        spread = spread + pltpu.roll(spread, 1, 0)
        dep_ref[:, cols] = shifted_ref[:, cols] * lax.rsqrt(1.0 + spread[0:4] / CHAN)
    copies[4].start()
    for copy in copies:
        copy.wait()


def body(radiances, band, row_in_band, column):
    vmem = pl.BlockSpec(memory_space=pltpu.VMEM)
    hbm = pl.BlockSpec(memory_space=pltpu.HBM)
    shape = jax.ShapeDtypeStruct
    grid = (NCELL, WIDE)
    outs = (
        shape((4, COLS), jnp.int32),
        shape((CH, 4, COLS), F32),
        shape((CH, 4, COLS), F32),
        shape((4, COLS), F32),
        shape((CH, OBS), F32),
    )
    between = (
        *outs[:4],
        shape((CH, OBS), F32),
        shape((NROW, CAP), F32),
        shape((1, OBS), F32),
        shape((1, OBS), F32),
    )
    nsem = len(GROUPS) + 2 * len(BACK) + 1
    operands = (
        radiances,
        band.reshape(1, OBS),
        row_in_band.reshape(1, OBS),
        column.reshape(1, OBS),
    )
    made = pl.pallas_call(
        comm_kernel,
        out_shape=between,
        in_specs=[hbm] * 4,
        out_specs=(vmem,) * 8,
        scratch_shapes=[
            pltpu.VMEM((CH, OBS), F32),
            pltpu.VMEM((1, OBS), jnp.int32),
            pltpu.VMEM((1, OBS), jnp.int32),
            pltpu.VMEM((1, OBS), jnp.int32),
            pltpu.VMEM((16 * NROW, OBS), BF16),
            pltpu.VMEM((CAP, OBS), BF16),
            pltpu.VMEM((NROW, 8, CAP), F32),
            pltpu.VMEM((NROW, 8, CAP), F32),
            pltpu.VMEM((FIELDS, 22 * CAP), F32),
            pltpu.VMEM((WIDE, NROW * CAP), BF16),
            pltpu.VMEM((FIELDS * NCELL + 32, WIDE), F32),
            pltpu.VMEM((10 * NCELL, WIDE), BF16),
            pltpu.VMEM((NROW, CAP), F32),
            pltpu.VMEM((NROW, 8, CAP), F32),
            pltpu.VMEM((NROW, 8, CAP), F32),
            pltpu.VMEM(((NCHAN - 1) * NROW, CAP), F32),
            pltpu.VMEM((NCHAN, *grid), F32),
            pltpu.SemaphoreType.DMA((nsem,)),
            pltpu.SemaphoreType.DMA((nsem,)),
            pltpu.SemaphoreType.REGULAR,
            pltpu.SemaphoreType.DMA((4,)),
        ],
        compiler_params=pltpu.CompilerParams(
            collective_id=0, has_side_effects=True, vmem_limit_bytes=24 << 20
        ),
    )(*(pltpu.with_memory_space_constraint(x, pltpu.HBM) for x in operands))
    return pl.pallas_call(
        last_kernel,
        out_shape=outs,
        in_specs=[vmem] * 8,
        out_specs=(hbm,) * 5,
        scratch_shapes=[pltpu.VMEM((CH, OBS), F32), pltpu.SemaphoreType.DMA((5,))],
        compiler_params=pltpu.CompilerParams(vmem_limit_bytes=16 << 20),
    )(*made)


def solution(mesh):
    in_specs = (P("chan", "rows"), P("rows", None), P("rows"), P("rows"))
    out_specs = (
        P("rows", None),
        P("chan", "rows", None),
        P("chan", "rows", None),
        P("rows", None),
        P("chan", "rows"),
    )
    return jax.shard_map(body, mesh=mesh, in_specs=in_specs, out_specs=out_specs, check_vma=False)
```

```python
import functools

import jax
import jax.numpy as jnp
from jax import lax
from jax.experimental import pallas as pl
from jax.experimental.pallas import tpu as pltpu
from jax.sharding import PartitionSpec as P

CHAN = 16
COLS = 1440
NROW = 32
NCHAN = 4
CH = 4
OBS = 2048
CAP = 128
WIDE = 256
NCELL = 24
MESH = pl.DeviceIdType.MESH
F32 = jnp.float32
BF16 = jnp.bfloat16


def hops(offset):
    ring = (0, 1, 2, 1)
    return ring[offset >> 3] + ring[(offset >> 1) & 3]


NEAR = tuple(sorted(range(NROW), key=hops))
FAR = tuple(d for d in reversed(NEAR) if d)
GROUPS = (NEAR[0:8], NEAR[8:20], NEAR[20:28], NEAR[28:32])
BACK = (NEAR,)
FIELDS = 16


def iota(shape, dim):
    return lax.broadcasted_iota(jnp.int32, shape, dim)


def rows16(row):
    return jnp.broadcast_to(row, (16, row.shape[1])).astype(BF16)


def count16(lanes):
    return iota((16, lanes), 0).astype(F32).astype(BF16)


def hot_into(ref, top, cols, names, blocks, lanes, first=0):
    one, zero = jnp.ones((16, lanes), BF16), jnp.zeros((16, lanes), BF16)
    steps = count16(lanes)
    for k in range(blocks):
        ref[top + 16 * k : top + 16 * k + 16, cols] = jnp.where(
            names == steps + jnp.asarray(16 * k + first, BF16), one, zero
        )


def high_of(x):
    return x.astype(BF16).astype(F32)


def spread_into_slots(radiances, bands, rib, column, left, right, rank_ref, tiles):
    lanes = OBS
    names = rows16(bands)
    hot_into(right, 0, slice(0, lanes), names, 2, lanes)
    blocks = [right[0:32, WIDE * j : WIDE * j + WIDE] for j in range(OBS // WIDE)]
    before, seen = [], jnp.zeros((32, WIDE), BF16)
    for block in blocks:
        before.append(seen)
        seen = seen + block
    stacked = jnp.concatenate(
        [jnp.concatenate(before, axis=0), jnp.concatenate(blocks, axis=0)], axis=1
    )
    ones = jnp.ones((WIDE, WIDE), BF16)
    upper = jnp.where(iota((WIDE, WIDE), 0) <= iota((WIDE, WIDE), 1), 1.0, 0.0).astype(BF16)
    prefix = jnp.dot(
        stacked, jnp.concatenate([ones, upper], axis=0), preferred_element_type=F32
    )
    ranks = []
    for j, block in enumerate(blocks):
        own = block.astype(F32) * prefix[32 * j : 32 * j + 32]
        ranks.append(jnp.sum(own, axis=0, keepdims=True) - 1.0)
    rank = jnp.concatenate(ranks, axis=1)
    rank_ref[...] = rank
    hot_into(right, 0, slice(0, lanes), rows16(rank), CAP // 16, lanes)

    row = iota((8, lanes), 0)
    both = jnp.concatenate([radiances, radiances], axis=0)
    high = high_of(both)
    middle = high_of(both - high)
    low = both - high - middle
    cell_hi = jnp.broadcast_to(((column >> 8) * 4 + rib + 1).astype(F32), (8, lanes))
    cell_lo = jnp.broadcast_to((column & 255).astype(F32), (8, lanes))
    names_of = jnp.where(row == 4, cell_hi, jnp.where(row == 5, cell_lo, 0.0))
    payload = jnp.concatenate(
        [jnp.where(row < 4, high, middle), jnp.where(row < 4, low, names_of)], axis=0
    ).astype(BF16)
    zero = jnp.zeros((16, lanes), BF16)
    for b in range(NROW):
        left[16 * b : 16 * b + 16, :] = jnp.where(names == jnp.asarray(b, BF16), payload, zero)
    placed = lax.dot_general(
        left[...], right[...], (((1,), (1,)), ((), ())), preferred_element_type=F32
    ).reshape(NROW, 16, CAP)
    upper_half, lower_half = placed[:, :8], placed[:, 8:]
    tile_row = iota((NROW, 8, CAP), 1)
    total = upper_half + pltpu.roll(upper_half, 4, 1) + lower_half
    tiles[...] = jnp.where(
        tile_row < 4, total, lower_half * 256.0 + pltpu.roll(lower_half, 7, 1)
    )


def feature_rows(ref, f1, f2, lanes):
    first = jnp.broadcast_to(ref[f1 : f1 + 1, 0:lanes], (8, lanes))
    second = jnp.broadcast_to(ref[f2 : f2 + 1, 0:lanes], (8, lanes))
    return [
        jnp.concatenate(pair, axis=0).astype(BF16)
        for pair in ((first, first), (first, second), (second, second))
    ]


def hi_and_lo(fields):
    highs = [high_of(x) for x in fields]
    lows = [x - h for x, h in zip(fields, highs)]
    return jnp.concatenate(highs + lows, axis=0).astype(BF16)


def accumulate(arrived, group, rows, left, hot, cols):
    lanes = len(group) * CAP
    row = iota((8, lanes), 0)
    tile = jnp.concatenate([arrived[d] for d in group], axis=1)
    code = jnp.concatenate(
        [jnp.broadcast_to(arrived[d, 4:5], (8, CAP)) for d in group], axis=1
    )
    value = jnp.where(row < 4, tile, pltpu.roll(tile, 4, 0))
    square = value * value
    value_hi, square_hi = high_of(value), high_of(square)
    rows[0:8, 0:lanes] = jnp.where(row < 4, value_hi, value - value_hi)
    rows[8:16, 0:lanes] = jnp.where(row < 4, square_hi, square - square_hi)
    cell_hi = jnp.floor(code * (1.0 / 256.0))
    cell_lo = code - 256.0 * cell_hi
    hi16 = jnp.concatenate([cell_hi, cell_hi], axis=0).astype(BF16)
    lo16 = jnp.concatenate([cell_lo, cell_lo], axis=0).astype(BF16)
    step = iota((16, lanes), 0)
    names = (step + 1, jnp.where(step < 8, step + 17, step - 7), step + 9)
    masks = [hi16 == n.astype(F32).astype(BF16) for n in names]
    zero = jnp.zeros((16, lanes), BF16)
    for pair in range(FIELDS // 2):
        for i, source in enumerate(feature_rows(rows, 2 * pair, 2 * pair + 1, lanes)):
            at = 48 * pair + 16 * i
            left[at : at + 16, 0:lanes] = jnp.where(masks[i], source, zero)
    hot_into(left, FIELDS * NCELL, slice(0, lanes), hi16, 2, lanes, first=1)
    hot_into(hot, 0, cols, lo16, WIDE // 16, lanes)
    return lax.dot_general(
        left[0 : FIELDS * NCELL + 32, 0:lanes],
        hot[:, cols],
        (((1,), (1,)), ((), ())),
        preferred_element_type=F32,
    )


def comm_kernel(
    rad_hbm,
    band_hbm,
    rib_hbm,
    col_hbm,
    count_out,
    mean_out,
    var_out,
    spread_out,
    shifted_ref,
    slots_ref,
    rank_ref,
    brel,
    rad_ref,
    band_ref,
    rib_ref,
    col_ref,
    left,
    right,
    tiles,
    arrived,
    rows,
    hot,
    sums,
    table,
    spread_table,
    own,
    back,
    returned,
    partial,
    spreads,
    send_sem,
    recv_sem,
    ready_sem,
    load_sem,
):
    loads = [
        pltpu.make_async_copy(src, dst, load_sem.at[i])
        for i, (src, dst) in enumerate(
            ((band_hbm, band_ref), (rad_hbm, rad_ref), (rib_hbm, rib_ref), (col_hbm, col_ref))
        )
    ]
    for load in loads:
        load.start()
    me, mine = lax.axis_index("rows"), lax.axis_index("chan")
    peer = {d: lax.bitwise_xor(me, d) for d in range(NROW)}
    other = {k: lax.bitwise_xor(mine, k) for k in range(NCHAN)}
    barrier = pltpu.get_barrier_semaphore()
    for d in FAR:
        pl.semaphore_signal(barrier, 1, device_id={"rows": peer[d]}, device_id_type=MESH)
    for k in range(1, NCHAN):
        pl.semaphore_signal(barrier, 1, device_id={"chan": other[k]}, device_id_type=MESH)

    for load in loads:
        load.wait()
    bands = lax.bitwise_xor(band_ref[...], me).astype(F32)
    brel[...] = bands
    spread_into_slots(
        rad_ref[...], bands, rib_ref[...], col_ref[...], left, right, rank_ref, tiles
    )
    arrived[0] = tiles[0]
    pl.semaphore_wait(barrier, NROW - 1 + NCHAN - 1)

    def remote(src, dst, which, **to):
        return pltpu.make_async_remote_copy(
            src_ref=src,
            dst_ref=dst,
            send_sem=send_sem.at[which],
            recv_sem=recv_sem.at[which],
            device_id=to,
            device_id_type=MESH,
        )

    def group_of(d, groups):
        return [d in group for group in groups].index(True)

    def wait_tiles(buffer, group, which):
        part = buffer.at[pl.ds(0, len(group) - (0 in group)), pl.ds(0, 5)]
        remote(part, part, which, rows=me).wait()

    first_back = len(GROUPS)
    first_part = first_back + len(BACK)
    grid_sem = first_part + len(BACK)

    for d in FAR:
        remote(
            tiles.at[d, pl.ds(0, 5)],
            arrived.at[d, pl.ds(0, 5)],
            group_of(d, GROUPS),
            rows=peer[d],
        ).start()
    for k in range(1, NCHAN):
        pl.semaphore_signal(ready_sem, 1, device_id={"chan": other[k]}, device_id_type=MESH)

    start = 0
    for g, group in enumerate(GROUPS):
        if len(group) > (0 in group):
            wait_tiles(arrived, group, g)
        cols = slice(start, start + len(group) * CAP)
        part = accumulate(arrived, group, rows, left, hot, cols)
        start = cols.stop
        if g == 0:
            sums[...] = part
        elif g < len(GROUPS) - 1:
            sums[...] += part

    def field(f):
        at = slice(NCELL * f, NCELL * f + NCELL)
        return part[at] + sums[at]

    count = field(FIELDS)
    inverse = 1.0 / jnp.maximum(count, 1.0)
    means, variances = [], []
    for c in range(CH):
        mean = (field(c) + field(c + 4)) * inverse
        var = jnp.maximum((field(c + 8) + field(c + 12)) * inverse - mean * mean, 0.0)
        means.append(mean)
        variances.append(var)
    own_spread = (variances[0] + variances[1]) + (variances[2] + variances[3])
    spreads[0] = own_spread
    spread_table[...] = hi_and_lo([own_spread])

    def send_partial(d, k):
        remote(
            own.at[pl.ds(d, 1)],
            partial.at[pl.ds((k - 1) * NROW + d, 1)],
            first_part,
            rows=peer[d],
            chan=other[k],
        ).start()

    def send_back(d):
        remote(
            back.at[d, pl.ds(0, 5)], returned.at[d, pl.ds(0, 5)], first_back, rows=peer[d]
        ).start()

    order = [d for group in GROUPS for d in group]

    def look(table, group, t, nfield):
        lanes = len(group) * CAP
        looks = jnp.dot(
            table[...], hot[:, lanes * t : lanes * t + lanes], preferred_element_type=F32
        ).reshape(2 * nfield, NCELL, lanes)
        looks = looks[:nfield] + looks[nfield:]
        code = jnp.concatenate(
            [jnp.broadcast_to(arrived[d, 4:5], (8, CAP)) for d in group], axis=1
        )
        cell_hi = jnp.floor(code * (1.0 / 256.0))
        row = iota((8, lanes), 0)
        here = [cell_hi == (row + (8 * i + 1)).astype(F32) for i in range(NCELL // 8)]
        result = []
        for f in range(nfield):
            only = jnp.where(here[0], looks[f, 0:8], 0.0)
            for i in range(1, NCELL // 8):
                only = only + jnp.where(here[i], looks[f, 8 * i : 8 * i + 8], 0.0)
            only = only + pltpu.roll(only, 4, 0)
            only = only + pltpu.roll(only, 2, 0)
            result.append(only + pltpu.roll(only, 1, 0))
        return result

    turn = 8
    for t in reversed(range(NROW // turn)):
        group = order[turn * t : turn * t + turn]
        (looked,) = look(spread_table, group, t, 1)
        for i, d in enumerate(group):
            own[d : d + 1] = looked[0:1, CAP * i : CAP * i + CAP]
        if t == NROW // turn - 1:
            pl.semaphore_wait(ready_sem, NCHAN - 1)
        for k in (2, 1, 3):
            for d in reversed(group):
                send_partial(d, k)

    table[...] = hi_and_lo(means)
    turn = 8
    for t in reversed(range(NROW // turn)):
        group = order[turn * t : turn * t + turn]
        row = iota((8, turn * CAP), 0)
        looked = jnp.concatenate(
            [jnp.broadcast_to(own[d : d + 1], (8, CAP)) for d in group], axis=1
        )
        for f, mean in enumerate(look(table, group, t, CH)):
            looked = jnp.where(row == f, mean, looked)
        tile = jnp.concatenate([arrived[d] for d in group], axis=1)
        tile = jnp.where(row < 4, tile - looked, looked)
        for i, d in enumerate(group):
            back[d] = tile[:, CAP * i : CAP * i + CAP]
        for d in reversed(group):
            if d:
                send_back(d)
    for k in range(1, NCHAN):
        remote(spreads.at[0], spreads.at[k], grid_sem, chan=other[k]).start()

    def to_rows(part, out, grid):
        lo, hi = WIDE * part, min(WIDE * part + WIDE, COLS)
        out[:, lo:hi] = grid[4 * part : 4 * part + 4, 0 : hi - lo].astype(out.dtype)

    returned[0] = back[0]
    for part in range(6):
        to_rows(part, count_out, count)
        for c in range(CH):
            to_rows(part, mean_out.at[c], means[c])
            to_rows(part, var_out.at[c], variances[c])

    wait_tiles(returned, NEAR, first_back)
    packed = returned[...].reshape(NROW * 8, CAP)
    high = high_of(packed)
    pieces = jnp.concatenate([high, packed - high], axis=1).astype(BF16)
    lanes = 512
    for t in range(OBS // lanes):
        cols = slice(t * lanes, t * lanes + lanes)
        twice = jnp.concatenate([right[:, cols], right[:, cols]], axis=0)
        found = jnp.dot(pieces, twice, preferred_element_type=F32)
        names = jnp.broadcast_to(brel[:, cols], (8, lanes))
        total = jnp.zeros((8, lanes), F32)
        for d in range(NROW):
            total = total + jnp.where(names == float(d), found[8 * d : 8 * d + 8], 0.0)
        shifted_ref[:, cols] = total[0:4]
    for d in range(NROW):
        slots_ref[d : d + 1] = returned[d, 4:5]
    waited = spreads.at[pl.ds(1, NCHAN - 1)]
    remote(waited, waited, grid_sem, rows=me).wait()
    spread = (spreads[0] + spreads[1]) + (spreads[2] + spreads[3])
    for part in range(6):
        to_rows(part, spread_out, spread)
    remote(partial, partial, first_part, rows=me).wait()
    rest = (partial[0:NROW] + partial[NROW : 2 * NROW]) + partial[2 * NROW :]
    slots_ref[...] += rest


def last_kernel(
    count_ref,
    mean_ref,
    var_ref,
    spread_ref,
    shifted_ref,
    slots_ref,
    rank_ref,
    brel,
    count_hbm,
    mean_hbm,
    var_hbm,
    spread_hbm,
    dep_hbm,
    dep_ref,
    sem,
):
    pairs = (
        (mean_ref, mean_hbm),
        (var_ref, var_hbm),
        (count_ref, count_hbm),
        (spread_ref, spread_hbm),
        (dep_ref, dep_hbm),
    )
    copies = [
        pltpu.make_async_copy(src, dst, sem.at[i]) for i, (src, dst) in enumerate(pairs)
    ]
    for copy in copies[:4]:
        copy.start()
    table = [slots_ref[8 * i : 8 * i + 8] for i in range(NROW // 8)]
    row = iota((8, CAP), 0)
    for t in range(OBS // CAP):
        cols = slice(t * CAP, t * CAP + CAP)
        at = jnp.broadcast_to(rank_ref[:, cols], (8, CAP)).astype(jnp.int32)
        names = jnp.broadcast_to(brel[:, cols], (8, CAP)).astype(jnp.int32)
        spread = jnp.zeros((8, CAP), F32)
        for i, lines in enumerate(table):
            there = jnp.take_along_axis(lines, at, axis=1, mode="promise_in_bounds")
            spread = spread + jnp.where(names == row + 8 * i, there, 0.0)
        spread = spread + pltpu.roll(spread, 4, 0)
        spread = spread + pltpu.roll(spread, 2, 0)
        spread = spread + pltpu.roll(spread, 1, 0)
        dep_ref[:, cols] = shifted_ref[:, cols] * lax.rsqrt(1.0 + spread[0:4] / CHAN)
    copies[4].start()
    for copy in copies:
        copy.wait()


def body(radiances, band, row_in_band, column):
    vmem = pl.BlockSpec(memory_space=pltpu.VMEM)
    hbm = pl.BlockSpec(memory_space=pltpu.HBM)
    shape = jax.ShapeDtypeStruct
    grid = (NCELL, WIDE)
    outs = (
        shape((4, COLS), jnp.int32),
        shape((CH, 4, COLS), F32),
        shape((CH, 4, COLS), F32),
        shape((4, COLS), F32),
        shape((CH, OBS), F32),
    )
    between = (
        *outs[:4],
        shape((CH, OBS), F32),
        shape((NROW, CAP), F32),
        shape((1, OBS), F32),
        shape((1, OBS), F32),
    )
    nsem = len(GROUPS) + 2 * len(BACK) + 1
    operands = (
        radiances,
        band.reshape(1, OBS),
        row_in_band.reshape(1, OBS),
        column.reshape(1, OBS),
    )
    made = pl.pallas_call(
        comm_kernel,
        out_shape=between,
        in_specs=[hbm] * 4,
        out_specs=(vmem,) * 8,
        scratch_shapes=[
            pltpu.VMEM((CH, OBS), F32),
            pltpu.VMEM((1, OBS), jnp.int32),
            pltpu.VMEM((1, OBS), jnp.int32),
            pltpu.VMEM((1, OBS), jnp.int32),
            pltpu.VMEM((16 * NROW, OBS), BF16),
            pltpu.VMEM((CAP, OBS), BF16),
            pltpu.VMEM((NROW, 8, CAP), F32),
            pltpu.VMEM((NROW, 8, CAP), F32),
            pltpu.VMEM((FIELDS, 22 * CAP), F32),
            pltpu.VMEM((WIDE, NROW * CAP), BF16),
            pltpu.VMEM((FIELDS * NCELL + 32, WIDE), F32),
            pltpu.VMEM((8 * NCELL, WIDE), BF16),
            pltpu.VMEM((2 * NCELL, WIDE), BF16),
            pltpu.VMEM((NROW, CAP), F32),
            pltpu.VMEM((NROW, 8, CAP), F32),
            pltpu.VMEM((NROW, 8, CAP), F32),
            pltpu.VMEM(((NCHAN - 1) * NROW, CAP), F32),
            pltpu.VMEM((NCHAN, *grid), F32),
            pltpu.SemaphoreType.DMA((nsem,)),
            pltpu.SemaphoreType.DMA((nsem,)),
            pltpu.SemaphoreType.REGULAR,
            pltpu.SemaphoreType.DMA((4,)),
        ],
        compiler_params=pltpu.CompilerParams(
            collective_id=0, has_side_effects=True, vmem_limit_bytes=24 << 20
        ),
    )(*(pltpu.with_memory_space_constraint(x, pltpu.HBM) for x in operands))
    return pl.pallas_call(
        last_kernel,
        out_shape=outs,
        in_specs=[vmem] * 8,
        out_specs=(hbm,) * 5,
        scratch_shapes=[pltpu.VMEM((CH, OBS), F32), pltpu.SemaphoreType.DMA((5,))],
        compiler_params=pltpu.CompilerParams(vmem_limit_bytes=16 << 20),
    )(*made)


def solution(mesh):
    in_specs = (P("chan", "rows"), P("rows", None), P("rows"), P("rows"))
    out_specs = (
        P("rows", None),
        P("chan", "rows", None),
        P("chan", "rows", None),
        P("rows", None),
        P("chan", "rows"),
    )
    return jax.shard_map(body, mesh=mesh, in_specs=in_specs, out_specs=out_specs, check_vma=False)
```

```python
import functools

import jax
import jax.numpy as jnp
from jax import lax
from jax.experimental import pallas as pl
from jax.experimental.pallas import tpu as pltpu
from jax.sharding import PartitionSpec as P

CHAN = 16
COLS = 1440
NROW = 32
NCHAN = 4
CH = 4
OBS = 2048
CAP = 128
WIDE = 256
NCELL = 24
MESH = pl.DeviceIdType.MESH
F32 = jnp.float32
BF16 = jnp.bfloat16


def hops(offset):
    ring = (0, 1, 2, 1)
    return ring[offset >> 3] + ring[(offset >> 1) & 3]


NEAR = tuple(sorted(range(NROW), key=hops))
FAR = tuple(d for d in reversed(NEAR) if d)
GROUPS = (NEAR[0:8], NEAR[8:20], NEAR[20:28], NEAR[28:32])
BACK = (NEAR,)
FIELDS = 16


def iota(shape, dim):
    return lax.broadcasted_iota(jnp.int32, shape, dim)


def rows16(row):
    return jnp.broadcast_to(row, (16, row.shape[1])).astype(BF16)


def count16(lanes):
    return iota((16, lanes), 0).astype(F32).astype(BF16)


def hot_into(ref, top, cols, names, blocks, lanes, first=0):
    one, zero = jnp.ones((16, lanes), BF16), jnp.zeros((16, lanes), BF16)
    steps = count16(lanes)
    for k in range(blocks):
        ref[top + 16 * k : top + 16 * k + 16, cols] = jnp.where(
            names == steps + jnp.asarray(16 * k + first, BF16), one, zero
        )


def high_of(x):
    return x.astype(BF16).astype(F32)


def spread_into_slots(radiances, bands, rib, column, left, right, rank_ref, tiles):
    lanes = OBS
    names = rows16(bands)
    hot_into(right, 0, slice(0, lanes), names, 2, lanes)
    blocks = [right[0:32, WIDE * j : WIDE * j + WIDE] for j in range(OBS // WIDE)]
    before, seen = [], jnp.zeros((32, WIDE), BF16)
    for block in blocks:
        before.append(seen)
        seen = seen + block
    stacked = jnp.concatenate(
        [jnp.concatenate(before, axis=0), jnp.concatenate(blocks, axis=0)], axis=1
    )
    ones = jnp.ones((WIDE, WIDE), BF16)
    upper = jnp.where(iota((WIDE, WIDE), 0) <= iota((WIDE, WIDE), 1), 1.0, 0.0).astype(BF16)
    prefix = jnp.dot(
        stacked, jnp.concatenate([ones, upper], axis=0), preferred_element_type=F32
    )
    ranks = []
    for j, block in enumerate(blocks):
        own = block.astype(F32) * prefix[32 * j : 32 * j + 32]
        ranks.append(jnp.sum(own, axis=0, keepdims=True) - 1.0)
    rank = jnp.concatenate(ranks, axis=1)
    rank_ref[...] = rank
    hot_into(right, 0, slice(0, lanes), rows16(rank), CAP // 16, lanes)

    row = iota((8, lanes), 0)
    both = jnp.concatenate([radiances, radiances], axis=0)
    high = high_of(both)
    middle = high_of(both - high)
    low = both - high - middle
    cell_hi = jnp.broadcast_to(((column >> 8) * 4 + rib + 1).astype(F32), (8, lanes))
    cell_lo = jnp.broadcast_to((column & 255).astype(F32), (8, lanes))
    names_of = jnp.where(row == 4, cell_hi, jnp.where(row == 5, cell_lo, 0.0))
    payload = jnp.concatenate(
        [jnp.where(row < 4, high, middle), jnp.where(row < 4, low, names_of)], axis=0
    ).astype(BF16)
    zero = jnp.zeros((16, lanes), BF16)
    for b in range(NROW):
        left[16 * b : 16 * b + 16, :] = jnp.where(names == jnp.asarray(b, BF16), payload, zero)
    placed = lax.dot_general(
        left[...], right[...], (((1,), (1,)), ((), ())), preferred_element_type=F32
    ).reshape(NROW, 16, CAP)
    upper_half, lower_half = placed[:, :8], placed[:, 8:]
    tile_row = iota((NROW, 8, CAP), 1)
    total = upper_half + pltpu.roll(upper_half, 4, 1) + lower_half
    tiles[...] = jnp.where(
        tile_row < 4, total, lower_half * 256.0 + pltpu.roll(lower_half, 7, 1)
    )


def feature_rows(ref, f1, f2, lanes):
    first = jnp.broadcast_to(ref[f1 : f1 + 1, 0:lanes], (8, lanes))
    second = jnp.broadcast_to(ref[f2 : f2 + 1, 0:lanes], (8, lanes))
    return [
        jnp.concatenate(pair, axis=0).astype(BF16)
        for pair in ((first, first), (first, second), (second, second))
    ]


def hi_and_lo(fields):
    highs = [high_of(x) for x in fields]
    lows = [x - h for x, h in zip(fields, highs)]
    return jnp.concatenate(highs + lows, axis=0).astype(BF16)


def accumulate(arrived, group, rows, left, hot, cols):
    lanes = len(group) * CAP
    row = iota((8, lanes), 0)
    tile = jnp.concatenate([arrived[d] for d in group], axis=1)
    code = jnp.concatenate(
        [jnp.broadcast_to(arrived[d, 4:5], (8, CAP)) for d in group], axis=1
    )
    value = jnp.where(row < 4, tile, pltpu.roll(tile, 4, 0))
    square = value * value
    value_hi, square_hi = high_of(value), high_of(square)
    rows[0:8, 0:lanes] = jnp.where(row < 4, value_hi, value - value_hi)
    rows[8:16, 0:lanes] = jnp.where(row < 4, square_hi, square - square_hi)
    cell_hi = jnp.floor(code * (1.0 / 256.0))
    cell_lo = code - 256.0 * cell_hi
    hi16 = jnp.concatenate([cell_hi, cell_hi], axis=0).astype(BF16)
    lo16 = jnp.concatenate([cell_lo, cell_lo], axis=0).astype(BF16)
    step = iota((16, lanes), 0)
    names = (step + 1, jnp.where(step < 8, step + 17, step - 7), step + 9)
    masks = [hi16 == n.astype(F32).astype(BF16) for n in names]
    zero = jnp.zeros((16, lanes), BF16)
    for pair in range(FIELDS // 2):
        for i, source in enumerate(feature_rows(rows, 2 * pair, 2 * pair + 1, lanes)):
            at = 48 * pair + 16 * i
            left[at : at + 16, 0:lanes] = jnp.where(masks[i], source, zero)
    hot_into(left, FIELDS * NCELL, slice(0, lanes), hi16, 2, lanes, first=1)
    hot_into(hot, 0, cols, lo16, WIDE // 16, lanes)
    return lax.dot_general(
        left[0 : FIELDS * NCELL + 32, 0:lanes],
        hot[:, cols],
        (((1,), (1,)), ((), ())),
        preferred_element_type=F32,
    )


def comm_kernel(
    rad_hbm,
    band_hbm,
    rib_hbm,
    col_hbm,
    count_out,
    mean_out,
    var_out,
    spread_out,
    shifted_ref,
    slots_ref,
    rank_ref,
    brel,
    rad_ref,
    band_ref,
    rib_ref,
    col_ref,
    left,
    right,
    tiles,
    arrived,
    rows,
    hot,
    sums,
    table,
    spread_table,
    own,
    back,
    returned,
    partial,
    spreads,
    send_sem,
    recv_sem,
    ready_sem,
    load_sem,
):
    loads = [
        pltpu.make_async_copy(src, dst, load_sem.at[i])
        for i, (src, dst) in enumerate(
            ((band_hbm, band_ref), (rad_hbm, rad_ref), (rib_hbm, rib_ref), (col_hbm, col_ref))
        )
    ]
    for load in loads:
        load.start()
    me, mine = lax.axis_index("rows"), lax.axis_index("chan")
    peer = {d: lax.bitwise_xor(me, d) for d in range(NROW)}
    other = {k: lax.bitwise_xor(mine, k) for k in range(NCHAN)}
    barrier = pltpu.get_barrier_semaphore()
    for d in FAR:
        pl.semaphore_signal(barrier, 1, device_id={"rows": peer[d]}, device_id_type=MESH)
    for k in range(1, NCHAN):
        pl.semaphore_signal(barrier, 1, device_id={"chan": other[k]}, device_id_type=MESH)

    for load in loads:
        load.wait()
    bands = lax.bitwise_xor(band_ref[...], me).astype(F32)
    brel[...] = bands
    spread_into_slots(
        rad_ref[...], bands, rib_ref[...], col_ref[...], left, right, rank_ref, tiles
    )
    arrived[0] = tiles[0]
    pl.semaphore_wait(barrier, NROW - 1 + NCHAN - 1)

    def remote(src, dst, which, **to):
        return pltpu.make_async_remote_copy(
            src_ref=src,
            dst_ref=dst,
            send_sem=send_sem.at[which],
            recv_sem=recv_sem.at[which],
            device_id=to,
            device_id_type=MESH,
        )

    def group_of(d, groups):
        return [d in group for group in groups].index(True)

    def wait_tiles(buffer, group, which):
        part = buffer.at[pl.ds(0, len(group) - (0 in group)), pl.ds(0, 5)]
        remote(part, part, which, rows=me).wait()

    first_back = len(GROUPS)
    first_part = first_back + len(BACK)
    grid_sem = first_part + len(BACK)

    for d in FAR:
        remote(
            tiles.at[d, pl.ds(0, 5)],
            arrived.at[d, pl.ds(0, 5)],
            group_of(d, GROUPS),
            rows=peer[d],
        ).start()
    for k in range(1, NCHAN):
        pl.semaphore_signal(ready_sem, 1, device_id={"chan": other[k]}, device_id_type=MESH)

    start = 0
    for g, group in enumerate(GROUPS):
        if len(group) > (0 in group):
            wait_tiles(arrived, group, g)
        cols = slice(start, start + len(group) * CAP)
        part = accumulate(arrived, group, rows, left, hot, cols)
        start = cols.stop
        if g == 0:
            sums[...] = part
        elif g < len(GROUPS) - 1:
            sums[...] += part

    def field(f):
        at = slice(NCELL * f, NCELL * f + NCELL)
        return part[at] + sums[at]

    count = field(FIELDS)
    inverse = 1.0 / jnp.maximum(count, 1.0)
    means, variances = [], []
    for c in range(CH):
        mean = (field(c) + field(c + 4)) * inverse
        var = jnp.maximum((field(c + 8) + field(c + 12)) * inverse - mean * mean, 0.0)
        means.append(mean)
        variances.append(var)
    own_spread = (variances[0] + variances[1]) + (variances[2] + variances[3])
    spreads[0] = own_spread
    spread_table[...] = hi_and_lo([own_spread])

    def send_partial(d, k):
        remote(
            own.at[pl.ds(d, 1)],
            partial.at[pl.ds((k - 1) * NROW + d, 1)],
            first_part,
            rows=peer[d],
            chan=other[k],
        ).start()

    def send_back(d):
        remote(
            back.at[d, pl.ds(0, 5)], returned.at[d, pl.ds(0, 5)], first_back, rows=peer[d]
        ).start()

    order = [d for group in GROUPS for d in group]

    def look(table, group, t, nfield):
        lanes = len(group) * CAP
        looks = jnp.dot(
            table[...], hot[:, lanes * t : lanes * t + lanes], preferred_element_type=F32
        ).reshape(2 * nfield, NCELL, lanes)
        looks = looks[:nfield] + looks[nfield:]
        code = jnp.concatenate(
            [jnp.broadcast_to(arrived[d, 4:5], (8, CAP)) for d in group], axis=1
        )
        cell_hi = jnp.floor(code * (1.0 / 256.0))
        row = iota((8, lanes), 0)
        here = [cell_hi == (row + (8 * i + 1)).astype(F32) for i in range(NCELL // 8)]
        result = []
        for f in range(nfield):
            only = jnp.where(here[0], looks[f, 0:8], 0.0)
            for i in range(1, NCELL // 8):
                only = only + jnp.where(here[i], looks[f, 8 * i : 8 * i + 8], 0.0)
            only = only + pltpu.roll(only, 4, 0)
            only = only + pltpu.roll(only, 2, 0)
            result.append(only + pltpu.roll(only, 1, 0))
        return result

    turn = 4
    for t in reversed(range(NROW // turn)):
        group = order[turn * t : turn * t + turn]
        (looked,) = look(spread_table, group, t, 1)
        for i, d in enumerate(group):
            own[d : d + 1] = looked[0:1, CAP * i : CAP * i + CAP]
        if t == NROW // turn - 1:
            pl.semaphore_wait(ready_sem, NCHAN - 1)
        for k in (2, 1, 3):
            for d in reversed(group):
                send_partial(d, k)

    table[...] = hi_and_lo(means)
    turn = 8
    for t in reversed(range(NROW // turn)):
        group = order[turn * t : turn * t + turn]
        row = iota((8, turn * CAP), 0)
        looked = jnp.concatenate(
            [jnp.broadcast_to(own[d : d + 1], (8, CAP)) for d in group], axis=1
        )
        for f, mean in enumerate(look(table, group, t, CH)):
            looked = jnp.where(row == f, mean, looked)
        tile = jnp.concatenate([arrived[d] for d in group], axis=1)
        tile = jnp.where(row < 4, tile - looked, looked)
        for i, d in enumerate(group):
            back[d] = tile[:, CAP * i : CAP * i + CAP]
        for d in reversed(group):
            if d:
                send_back(d)
    for k in range(1, NCHAN):
        remote(spreads.at[0], spreads.at[k], grid_sem, chan=other[k]).start()

    def to_rows(part, out, grid):
        lo, hi = WIDE * part, min(WIDE * part + WIDE, COLS)
        out[:, lo:hi] = grid[4 * part : 4 * part + 4, 0 : hi - lo].astype(out.dtype)

    returned[0] = back[0]
    for part in range(6):
        to_rows(part, count_out, count)
        for c in range(CH):
            to_rows(part, mean_out.at[c], means[c])
            to_rows(part, var_out.at[c], variances[c])

    wait_tiles(returned, NEAR, first_back)
    packed = returned[...].reshape(NROW * 8, CAP)
    high = high_of(packed)
    pieces = jnp.concatenate([high, packed - high], axis=1).astype(BF16)
    lanes = 512
    for t in range(OBS // lanes):
        cols = slice(t * lanes, t * lanes + lanes)
        twice = jnp.concatenate([right[:, cols], right[:, cols]], axis=0)
        found = jnp.dot(pieces, twice, preferred_element_type=F32)
        names = jnp.broadcast_to(brel[:, cols], (8, lanes))
        total = jnp.zeros((8, lanes), F32)
        for d in range(NROW):
            total = total + jnp.where(names == float(d), found[8 * d : 8 * d + 8], 0.0)
        shifted_ref[:, cols] = total[0:4]
    for d in range(NROW):
        slots_ref[d : d + 1] = returned[d, 4:5]
    waited = spreads.at[pl.ds(1, NCHAN - 1)]
    remote(waited, waited, grid_sem, rows=me).wait()
    spread = (spreads[0] + spreads[1]) + (spreads[2] + spreads[3])
    for part in range(6):
        to_rows(part, spread_out, spread)
    remote(partial, partial, first_part, rows=me).wait()
    rest = (partial[0:NROW] + partial[NROW : 2 * NROW]) + partial[2 * NROW :]
    slots_ref[...] += rest


def last_kernel(
    count_ref,
    mean_ref,
    var_ref,
    spread_ref,
    shifted_ref,
    slots_ref,
    rank_ref,
    brel,
    count_hbm,
    mean_hbm,
    var_hbm,
    spread_hbm,
    dep_hbm,
    dep_ref,
    sem,
):
    pairs = (
        (mean_ref, mean_hbm),
        (var_ref, var_hbm),
        (count_ref, count_hbm),
        (spread_ref, spread_hbm),
        (dep_ref, dep_hbm),
    )
    copies = [
        pltpu.make_async_copy(src, dst, sem.at[i]) for i, (src, dst) in enumerate(pairs)
    ]
    for copy in copies[:4]:
        copy.start()
    table = [slots_ref[8 * i : 8 * i + 8] for i in range(NROW // 8)]
    row = iota((8, CAP), 0)
    for t in range(OBS // CAP):
        cols = slice(t * CAP, t * CAP + CAP)
        at = jnp.broadcast_to(rank_ref[:, cols], (8, CAP)).astype(jnp.int32)
        names = jnp.broadcast_to(brel[:, cols], (8, CAP)).astype(jnp.int32)
        spread = jnp.zeros((8, CAP), F32)
        for i, lines in enumerate(table):
            there = jnp.take_along_axis(lines, at, axis=1, mode="promise_in_bounds")
            spread = spread + jnp.where(names == row + 8 * i, there, 0.0)
        spread = spread + pltpu.roll(spread, 4, 0)
        spread = spread + pltpu.roll(spread, 2, 0)
        spread = spread + pltpu.roll(spread, 1, 0)
        dep_ref[:, cols] = shifted_ref[:, cols] * lax.rsqrt(1.0 + spread[0:4] / CHAN)
    copies[4].start()
    for copy in copies:
        copy.wait()


def body(radiances, band, row_in_band, column):
    vmem = pl.BlockSpec(memory_space=pltpu.VMEM)
    hbm = pl.BlockSpec(memory_space=pltpu.HBM)
    shape = jax.ShapeDtypeStruct
    grid = (NCELL, WIDE)
    outs = (
        shape((4, COLS), jnp.int32),
        shape((CH, 4, COLS), F32),
        shape((CH, 4, COLS), F32),
        shape((4, COLS), F32),
        shape((CH, OBS), F32),
    )
    between = (
        *outs[:4],
        shape((CH, OBS), F32),
        shape((NROW, CAP), F32),
        shape((1, OBS), F32),
        shape((1, OBS), F32),
    )
    nsem = len(GROUPS) + 2 * len(BACK) + 1
    operands = (
        radiances,
        band.reshape(1, OBS),
        row_in_band.reshape(1, OBS),
        column.reshape(1, OBS),
    )
    made = pl.pallas_call(
        comm_kernel,
        out_shape=between,
        in_specs=[hbm] * 4,
        out_specs=(vmem,) * 8,
        scratch_shapes=[
            pltpu.VMEM((CH, OBS), F32),
            pltpu.VMEM((1, OBS), jnp.int32),
            pltpu.VMEM((1, OBS), jnp.int32),
            pltpu.VMEM((1, OBS), jnp.int32),
            pltpu.VMEM((16 * NROW, OBS), BF16),
            pltpu.VMEM((CAP, OBS), BF16),
            pltpu.VMEM((NROW, 8, CAP), F32),
            pltpu.VMEM((NROW, 8, CAP), F32),
            pltpu.VMEM((FIELDS, 22 * CAP), F32),
            pltpu.VMEM((WIDE, NROW * CAP), BF16),
            pltpu.VMEM((FIELDS * NCELL + 32, WIDE), F32),
            pltpu.VMEM((8 * NCELL, WIDE), BF16),
            pltpu.VMEM((2 * NCELL, WIDE), BF16),
            pltpu.VMEM((NROW, CAP), F32),
            pltpu.VMEM((NROW, 8, CAP), F32),
            pltpu.VMEM((NROW, 8, CAP), F32),
            pltpu.VMEM(((NCHAN - 1) * NROW, CAP), F32),
            pltpu.VMEM((NCHAN, *grid), F32),
            pltpu.SemaphoreType.DMA((nsem,)),
            pltpu.SemaphoreType.DMA((nsem,)),
            pltpu.SemaphoreType.REGULAR,
            pltpu.SemaphoreType.DMA((4,)),
        ],
        compiler_params=pltpu.CompilerParams(
            collective_id=0, has_side_effects=True, vmem_limit_bytes=24 << 20
        ),
    )(*(pltpu.with_memory_space_constraint(x, pltpu.HBM) for x in operands))
    return pl.pallas_call(
        last_kernel,
        out_shape=outs,
        in_specs=[vmem] * 8,
        out_specs=(hbm,) * 5,
        scratch_shapes=[pltpu.VMEM((CH, OBS), F32), pltpu.SemaphoreType.DMA((5,))],
        compiler_params=pltpu.CompilerParams(vmem_limit_bytes=16 << 20),
    )(*made)


def solution(mesh):
    in_specs = (P("chan", "rows"), P("rows", None), P("rows"), P("rows"))
    out_specs = (
        P("rows", None),
        P("chan", "rows", None),
        P("chan", "rows", None),
        P("rows", None),
        P("chan", "rows"),
    )
    return jax.shard_map(body, mesh=mesh, in_specs=in_specs, out_specs=out_specs, check_vma=False)
```
